256 devices in a mesh: panel: 4 (over x_hi, core), tile: 64 (over y, x_lo, z).
Axes of the slice: x: 4 (x_hi: 2, x_lo: 2; x = x_hi * 2 + x_lo), y: 4, z: 8, core: 2. Of those that a mesh axis runs over, the one named last changes fastest.
Arguments:
- residual: float32 [4, 64, 128, 8, 128], P('panel', 'tile'), may hold values from -6 to 6
- inverse: bfloat16 [4, 64, 16, 576, 576], P('panel', 'tile'), may hold values from -1 to 2
- blend_weight: float32 [576], replicated, may hold values from 0.1 to 1.9
- seam_table: int32 [4, 4, 3], replicated, may hold values from -1 to 3, as said below
Outputs:
- correction: float32 [4, 64, 128, 8, 128], P('panel', 'tile')
The draws below stay inside these ranges and needn't reach their ends.
Inputs may be any that keep to these rules, and one draw needn't show every extreme that they name: seam_table[p, e] holds the neighbour panel across edge e of panel p (or -1), a rotation r and a reversal v. Every panel has neighbours across exactly two opposite edges (0 and 2, or 1 and 3) and the entries -1, 0, 0 on the other two; the panels form one closed cycle and each panel's two neighbours differ. If edge e of p faces panel q, then edge c = (e + 2 + r) mod 4 of q faces p with rotation (-r) mod 4 and the same reversal v. At least one seam joins edge 0 of a panel to edge 0 of another, with rotation 2 and reversal 1.
All inputs are finite; a program needn't handle non-finite values.
Results may differ from the reference program's by a relative error of at most 0.0029.
Values may be sent and summed in bfloat16 or wider, within the bound.
A program may use at most 128 MiB of HBM per device.

```python
import math
import jax
import jax.numpy as jnp
from jax import lax

PANELS = 4
SUB = 8
INTERSECTION = 8
COLS = 128
TILES = 64
TILE_COLS = 32
TILE_W = 8
TILE_H = 128
NSUB = 16
CELLS = 576


def draw_inverse(key, part):
    matrix_order = CELLS

    def one_block(tile_index):
        sub_key = jax.random.fold_in(key, tile_index)
        noise_part = jax.random.normal(jax.random.fold_in(sub_key, 3), (NSUB, matrix_order, matrix_order), jnp.float32)
        noise_part = noise_part * (0.6 / math.sqrt(matrix_order))
        diagonal = jax.random.uniform(jax.random.fold_in(sub_key, 4), (NSUB, matrix_order), jnp.float32, 0.5, 1.5)
        result = noise_part + diagonal[:, :, None] * jnp.eye(matrix_order, dtype=jnp.float32)[None]
        return result.astype(jnp.bfloat16)
    blocks = lax.map(one_block, jnp.arange(PANELS * TILES, dtype=jnp.int32))
    return blocks.reshape(PANELS, TILES, NSUB, matrix_order, matrix_order)


def draw_seam_table(key, part):
    ordering = jax.random.permutation(jax.random.fold_in(key, 1), PANELS).astype(jnp.int32)
    rotations = jax.random.randint(jax.random.fold_in(key, 2), (PANELS,), 0, 4).astype(jnp.int32)
    rotations = rotations.at[ordering[0]].set(2)
    rotations = rotations.at[ordering[1]].set(0)
    direction = jnp.array([1, -1, -1, 1], jnp.int32)
    seam_grid = jnp.zeros((PANELS, 4, 3), jnp.int32).at[:, :, 0].set(-1)
    for position in range(PANELS):
        current = ordering[position]
        following = ordering[(position + 1) % PANELS]
        east_edge = (2 + rotations[current]) % 4
        west_edge = rotations[following] % 4
        reversal = (direction[rotations[current]] != direction[rotations[following]]).astype(jnp.int32)
        seam_grid = seam_grid.at[current, east_edge].set(jnp.stack([following, (west_edge - east_edge - 2) % 4, reversal]))
        seam_grid = seam_grid.at[following, west_edge].set(jnp.stack([current, (east_edge - west_edge - 2) % 4, reversal]))
    return seam_grid


def steps_of(own_key, dims, shards, least, top_value):
    level = 1.0
    for dim, blocks in shards:
        steps = jax.random.uniform(jax.random.fold_in(jax.random.fold_in(own_key, 6), dim), (blocks,), jnp.float32, least / len(shards), top_value / len(shards))
        level = level * jnp.repeat(jnp.exp(steps), dims[dim] // blocks).reshape((-1,) + (1,) * (len(dims) - 1 - dim))
    return level


def bell_draw(key, extent, scale, limit, cuts=(), held_as=jnp.bfloat16):
    values = jax.random.normal(key, extent, jnp.float32) * scale
    if len(cuts) > 0:
        values = steps_of(key, extent, cuts, -0.22, 0.18) * values
    return jnp.clip(values, min=-limit, max=limit).astype(held_as)


def setup_inputs(seed: int = 0) -> dict:
    splits = jax.random.split(jax.random.key(seed), 5)
    residual = bell_draw(splits[0], (PANELS, TILES, TILE_H, TILE_W, COLS), 1.0, 6.0, ((0, 4), (1, 64)), jnp.float32)
    inverse = draw_inverse(jax.random.fold_in(splits[4], 71), 0)
    blend_weight = jnp.clip(1.0 + 0.18 * jax.random.normal(splits[2], (CELLS,), jnp.float32), 0.1, 1.9)
    seam_table = draw_seam_table(jax.random.fold_in(splits[4], 71), 0)
    return {"residual": residual, "inverse": inverse, "blend_weight": blend_weight, "seam_table": seam_table}


def edge_strip(values, edge_id):
    margin = INTERSECTION
    if edge_id == 0:
        return jnp.transpose(values[:, :margin], (1, 0, 2))
    if edge_id == 1:
        return values[:margin]
    if edge_id == 2:
        return jnp.transpose(values[:, ::-1][:, :margin], (1, 0, 2))
    return values[::-1][:margin]


def incoming(strips, seam_table, panel_id, edge_id):
    seam_entry = seam_table[panel_id, edge_id]
    neighbour = jnp.maximum(seam_entry[0], 0)
    facing = (edge_id + 2 + seam_entry[1]) % 4
    picked = strips[neighbour, facing]
    picked = jnp.where(seam_entry[2] > 0, picked[:, ::-1], picked)
    return jnp.where(seam_entry[0] >= 0, picked, jnp.zeros_like(picked))


def with_ghosts(values, ghost_sets):
    margin = INTERSECTION
    widened = [jnp.pad(band, ((0, 0), (margin, margin), (0, 0))) for band in ghost_sets]
    padded = jnp.pad(values, ((margin, margin), (margin, margin), (0, 0)))
    padded = padded.at[:, :margin].set(jnp.transpose(widened[0][::-1], (1, 0, 2)))
    padded = padded.at[:margin, :].set(widened[1][::-1])
    padded = padded.at[:, -margin:].set(jnp.transpose(widened[2], (1, 0, 2)))
    padded = padded.at[-margin:, :].set(widened[3])
    return padded


def ghost_bands(padded):
    margin = INTERSECTION
    interior = padded.shape[0] - 2 * margin
    western = jnp.transpose(padded[margin:margin + interior, :margin][:, ::-1], (1, 0, 2))
    southern = padded[:margin, margin:margin + interior][::-1]
    eastern = jnp.transpose(padded[margin:margin + interior, -margin:], (1, 0, 2))
    northern = padded[-margin:, margin:margin + interior]
    return [western, southern, eastern, northern]


def add_bands(values, ghost_sets):
    margin = INTERSECTION
    values = values.at[:, :margin].add(jnp.transpose(ghost_sets[0], (1, 0, 2)))
    values = values.at[:margin].add(ghost_sets[1])
    values = values.at[:, -margin:].add(jnp.transpose(ghost_sets[2][::-1], (1, 0, 2)))
    values = values.at[-margin:].add(ghost_sets[3][::-1])
    return values


def patches(padded, block_rows, block_cols):
    columns = padded.shape[-1]
    blocked = padded.reshape(block_rows + 2, SUB, block_cols + 2, SUB, columns)
    pieces = [blocked[row_shift:row_shift + block_rows, :, col_shift:col_shift + block_cols]
              for row_shift in range(3) for col_shift in range(3)]
    stacked = jnp.stack(pieces).reshape(3, 3, block_rows, SUB, block_cols, SUB, columns)
    stacked = jnp.transpose(stacked, (2, 4, 0, 3, 1, 5, 6))
    return stacked.reshape(block_rows, block_cols, 9 * SUB * SUB, columns)


def intersection_add(solved, block_rows, block_cols):
    columns = solved.shape[-1]
    shaped = solved.reshape(block_rows, block_cols, 3, SUB, 3, SUB, columns)
    summed = jnp.zeros((block_rows + 2, SUB, block_cols + 2, SUB, columns), jnp.float32)
    for row_shift in range(3):
        for col_shift in range(3):
            block_part = jnp.transpose(shaped[:, :, row_shift, :, col_shift], (0, 2, 1, 3, 4))
            summed = summed.at[row_shift:row_shift + block_rows, :, col_shift:col_shift + block_cols].add(block_part)
    return summed.reshape((block_rows + 2) * SUB, (block_cols + 2) * SUB, columns)


def reference(residual, inverse, blend_weight, seam_table):
    margin = INTERSECTION
    tile_rows = residual.shape[1] // TILE_COLS
    height, tile_width, columns = residual.shape[2], residual.shape[3], residual.shape[4]
    panel_side = tile_width * TILE_COLS
    sub_rows, sub_cols = height // SUB, tile_width // SUB
    block_rows, block_cols = tile_rows * sub_rows, TILE_COLS * sub_cols
    cells = 9 * SUB * SUB
    panel_grid = residual.reshape(PANELS, tile_rows, TILE_COLS, height, tile_width, columns)
    panel_grid = jnp.transpose(panel_grid, (0, 1, 3, 2, 4, 5)).reshape(PANELS, panel_side, panel_side, columns)
    source = panel_grid.astype(jnp.bfloat16)
    strips = jnp.stack([jnp.stack([edge_strip(source[panel_id], edge_id) for edge_id in range(4)])
                        for panel_id in range(PANELS)])
    vectors = []
    for panel_id in range(PANELS):
        padded = with_ghosts(source[panel_id], [incoming(strips, seam_table, panel_id, edge_id) for edge_id in range(4)])
        local_patches = patches(padded, block_rows, block_cols)
        local_patches = local_patches.reshape(tile_rows, sub_rows, TILE_COLS, sub_cols, cells, columns)
        local_patches = jnp.transpose(local_patches, (0, 2, 1, 3, 4, 5))
        vectors.append(local_patches.reshape(tile_rows * TILE_COLS, sub_rows * sub_cols, cells, columns))
    vectors = jnp.stack(vectors)
    tile_count = PANELS * tile_rows * TILE_COLS

    def solve(operands):
        return jnp.einsum("noi,nir->nor", operands[0].astype(jnp.float32), operands[1].astype(jnp.float32))

    solved = lax.map(solve, (inverse.reshape((tile_count,) + inverse.shape[2:]),
                             vectors.reshape((tile_count,) + vectors.shape[2:])))
    solved = solved * blend_weight[None, None, :, None]
    solved = solved.reshape(PANELS, tile_rows, TILE_COLS, sub_rows, sub_cols, cells, columns)
    solved = jnp.transpose(solved, (0, 1, 3, 2, 4, 5, 6)).reshape(PANELS, block_rows, block_cols, cells, columns)
    spread = jnp.stack([intersection_add(solved[panel_id], block_rows, block_cols) for panel_id in range(PANELS)])
    ghost_sets = jnp.stack([jnp.stack(ghost_bands(spread[panel_id])) for panel_id in range(PANELS)])
    interior = spread[:, margin:margin + panel_side, margin:margin + panel_side]
    folded = jnp.stack([add_bands(interior[panel_id],
                                  [incoming(ghost_sets, seam_table, panel_id, edge_id) for edge_id in range(4)])
                        for panel_id in range(PANELS)])
    folded = folded.reshape(PANELS, tile_rows, height, TILE_COLS, tile_width, columns)
    return jnp.transpose(folded, (0, 1, 3, 2, 4, 5)).reshape(residual.shape)
```

```python
import functools

import jax
import jax.numpy as jnp
from jax import lax
from jax.experimental import pallas as pl
from jax.experimental.pallas import tpu as pltpu
from jax.sharding import PartitionSpec as P

PANELS = 4
TILE_COLS = 32
H = 128
LAST = TILE_COLS - 1
NSUB = 16
CELLS = 576
MESH = pl.DeviceIdType.MESH

SEND_COUNT = 80
RECV_COUNT = 80


def kernel(seam, res_hbm, inv_hbm, weight, out_hbm, res, inv, wrep, ext, spread, spb, out,
           s1buf, send_x, recv_x, row_buf, col_buf, yf, gf,
           from_left, from_right, from_vert, from_dl, from_dr,
           home_left, home_right, home_corner, send_b, recv_b, cb_buf, corner_in,
           local_sem, inv_sem, send_sem, recv_sem):
    panel = lax.axis_index("panel")
    tile = lax.axis_index("tile")
    r = tile // TILE_COLS
    c = tile % TILE_COLS
    other = 1 - r
    has_left = c > 0
    has_right = c < LAST
    at_end = jnp.logical_or(c == 0, c == LAST)
    side = jnp.where(c == LAST, 1, 0)
    half = c // 16
    is_self = jnp.logical_or(tile == 0, tile == 2 * TILE_COLS - 1)
    seam_rows = 136 * r
    inner_rows = 136 * other
    two_corners = jnp.logical_or(c == 15, c == 16)
    corner_tile = half * TILE_COLS + LAST * r
    other_corner = (1 - half) * TILE_COLS + LAST * r

    def tid(row, col):
        return row * TILE_COLS + col

    res_copy = pltpu.make_async_copy(res_hbm, res, local_sem.at[0])
    res_copy.start()
    for n in range(NSUB):
        pltpu.make_async_copy(inv_hbm.at[n], inv.at[n], inv_sem.at[n]).start()

    zero_block = jnp.zeros((8, 8, 128), jnp.bfloat16)

    @pl.when(at_end)
    def _():
        ext[pl.ds(seam_rows, 8), 2 * side] = zero_block

    home_corner[...] = jnp.zeros_like(home_corner)
    home_left[...] = zero_block
    home_right[...] = zero_block

    barrier = pltpu.get_barrier_semaphore()

    def greet(cond, pan, til):
        @pl.when(cond)
        def _():
            pl.semaphore_signal(barrier, inc=1, device_id=(pan, til), device_id_type=MESH)

    yes = tile >= 0
    greet(has_left, panel, tid(r, c - 1))
    greet(has_right, panel, tid(r, c + 1))
    greet(yes, panel, tid(other, c))
    greet(has_left, panel, tid(other, c - 1))
    greet(has_right, panel, tid(other, c + 1))
    for step in range(1, PANELS):
        q = lax.rem(panel + step, PANELS)
        for row in range(2):
            greet(yes, q, tid(row, c))
            greet(yes, q, tid(row, LAST - c))
    greet(jnp.logical_not(is_self), panel, corner_tile)
    greet(two_corners, panel, other_corner)
    for jj in range(18):
        k = 16 * r + jj - 1
        ok = jnp.logical_and(at_end, jnp.logical_and(k >= 0, k < TILE_COLS))
        ok = jnp.logical_and(ok, tid(side, k) != tile)
        greet(ok, panel, tid(side, k))

    res_copy.wait()
    ext[8:136, 1] = res[...].astype(jnp.bfloat16)

    count = 13 + 2 * has_left.astype(jnp.int32) + 2 * has_right.astype(jnp.int32)
    count = count + jnp.where(is_self, 0, 1) + jnp.where(two_corners, 1, 0)
    count = count + jnp.where(at_end, jnp.where(is_self, 16, 17), 0)
    pl.semaphore_wait(barrier, count)

    sends = []

    def remote(src, dst, slot, rslot, pan, til):
        return pltpu.make_async_remote_copy(
            src_ref=src, dst_ref=dst, send_sem=send_sem.at[slot], recv_sem=recv_sem.at[rslot],
            device_id=(pan, til), device_id_type=MESH)

    def send(cond, src, dst, slot, rslot, pan, til):
        @pl.when(cond)
        def _():
            remote(src, dst, slot, rslot, pan, til).start()
        sends.append((cond, src, dst, slot, rslot, pan, til))

    def arrived(cond, dst, rslot):
        @pl.when(cond)
        def _():
            remote(dst, dst, 0, rslot, panel, tile).wait_recv()

    for j in range(16):
        home = tid(side, 16 * r + j)
        ok = jnp.logical_and(at_end, home != tile)
        send(ok, ext.at[pl.ds(8 + 8 * j, 8), 1], s1buf, j, 0, panel, home)
    edge_src = ext.at[pl.ds(128 - 120 * r, 8), 1]
    send(yes, edge_src, ext.at[pl.ds(136 * r, 8), 1], 16, 1, panel, tid(other, c))
    send(has_right, edge_src, ext.at[pl.ds(136 * r, 8), 0], 17, 2, panel, tid(other, c + 1))
    send(has_left, edge_src, ext.at[pl.ds(136 * r, 8), 2], 18, 3, panel, tid(other, c - 1))
    mid = ext.at[pl.ds(8, 128), 1]
    send(has_right, mid, ext.at[pl.ds(8, 128), 0], 19, 4, panel, tid(r, c + 1))
    send(has_left, mid, ext.at[pl.ds(8, 128), 2], 20, 5, panel, tid(r, c - 1))

    row_type = jnp.where(seam[panel, 1, 0] >= 0, 1, 0)
    edge = 2 * r + row_type
    facing_panel = jnp.maximum(seam[panel, edge, 0], 0)
    rev = jnp.where(seam[panel, edge, 2] > 0, 1, 0)
    facing = lax.rem(edge + 2 + seam[panel, edge, 1], 4)
    facing_slot = jnp.where(facing >= 2, 1, 0)
    facing_row = facing - 2 * facing_slot
    delta = lax.rem(facing_panel - panel + 3, 4)
    delta = jnp.clip(delta, 0, 2)
    pick = (delta * 2 + facing_slot) * 2 + rev
    along = jnp.where(facing_row == 1, 1, 8)
    across = jnp.where(facing_row == 1, 8, 1)
    flip = jnp.where(facing_slot == r, 1, 0)
    along_step = along * (1 - 2 * rev)
    across_step = across * (1 - 2 * flip)
    start = along * 7 * rev + across * 7 * flip
    step_i = jnp.where(row_type == 1, across_step, along_step)
    step_j = jnp.where(row_type == 1, along_step, across_step)

    def turned(received):
        yf[...] = received[pick].astype(jnp.float32).reshape(64, 128)
        for i in range(8):
            for j in range(8):
                gf[pl.ds(8 * i + j, 1), :] = yf[pl.ds(start + step_i * i + step_j * j, 1), :]
        return gf[...].reshape(8, 8, 128)

    own_rows = ext[pl.ds(8 + 120 * r, 8), 1]

    @pl.when(is_self)
    def _():
        s1buf[...] = own_rows

    arrived(jnp.logical_not(is_self), s1buf, 0)
    rowf = jnp.full((8, 8, 128), row_type, jnp.int32) == 1
    send_x[...] = jnp.where(rowf, own_rows.astype(jnp.float32), s1buf[...].astype(jnp.float32)).astype(jnp.bfloat16)

    def across_panels(buf, landing, base, rbase):
        slot = 0
        for step in range(1, PANELS):
            q = lax.rem(panel + step, PANELS)
            for row in range(2):
                for v in range(2):
                    col = LAST - c if v else c
                    for own in range(2):
                        idx = ((3 - step) * 2 + own) * 2 + v
                        if own == 0:
                            send(jnp.logical_and(yes, r == 0), buf, landing.at[idx],
                                 base + slot, rbase + idx, q, tid(row, col))
                        else:
                            send(r == 1, buf, landing.at[idx],
                                 base + slot, rbase + idx, q, tid(row, col))
                    slot += 1
        for idx in range(12):
            arrived(yes, landing.at[idx], rbase + idx)

    across_panels(send_x, recv_x, 21, 6)
    turn = turned(recv_x)
    zero_f = jnp.zeros((8, 8, 128), jnp.float32)
    row_val = jnp.where(rowf, turn, zero_f).astype(jnp.bfloat16)
    row_buf[...] = row_val
    col_buf[...] = jnp.where(rowf, zero_f, turn).astype(jnp.bfloat16)
    pos = 8 + 8 * (c - 16 * half)
    send(jnp.logical_not(is_self), col_buf, ext.at[pl.ds(pos, 8), 2 * r], 33, 20 + c - 16 * half, panel, corner_tile)
    opos = 8 + 8 * (c - 16 * (1 - half))
    send(two_corners, col_buf, ext.at[pl.ds(opos, 8), 2 * r], 34, 20 + c - 16 * (1 - half), panel, other_corner)
    send(has_right, row_buf, ext.at[pl.ds(seam_rows, 8), 0], 35, 18, panel, tid(r, c + 1))
    send(has_left, row_buf, ext.at[pl.ds(seam_rows, 8), 2], 36, 37, panel, tid(r, c - 1))
    ext[pl.ds(seam_rows, 8), 1] = row_val

    @pl.when(is_self)
    def _():
        ext[pl.ds(pos, 8), 2 * r] = col_buf[...]

    wrep[...] = jnp.transpose(jnp.broadcast_to(weight[...], (128, CELLS)), (1, 0))
    spread[...] = jnp.zeros_like(spread)

    arrived(yes, ext.at[pl.ds(inner_rows, 8), 1], 1)
    arrived(has_left, ext.at[pl.ds(inner_rows, 8), 0], 2)
    arrived(has_right, ext.at[pl.ds(inner_rows, 8), 2], 3)
    arrived(has_left, ext.at[pl.ds(8, 128), 0], 4)
    arrived(has_right, ext.at[pl.ds(8, 128), 2], 5)
    arrived(has_left, ext.at[pl.ds(seam_rows, 8), 0], 18)
    arrived(has_right, ext.at[pl.ds(seam_rows, 8), 2], 37)
    for jj in range(18):
        k = 16 * r + jj - 1
        ok = jnp.logical_and(at_end, jnp.logical_and(k >= 0, k < TILE_COLS))
        ok = jnp.logical_and(ok, tid(side, k) != tile)
        arrived(ok, ext.at[pl.ds(8 * jj, 8), 2 * side], 19 + jj)

    flat = ext.reshape(144 * 24, 128)
    def solve(n, carry):
        pltpu.make_async_copy(inv_hbm.at[n], inv.at[n], inv_sem.at[n]).wait()
        rows = pl.ds(pl.multiple_of(n * 192, 64), CELLS)
        solved = jnp.dot(inv[n], flat[rows, :], preferred_element_type=jnp.float32)
        spread[rows, :] += solved * wrep[...]
        return carry

    lax.fori_loop(0, NSUB, solve, 0)

    cube = spread.reshape(144, 3, 8, 128)
    spb[...] = cube[...].astype(jnp.bfloat16)

    for jj in range(18):
        k = 16 * r + jj - 1
        ok = jnp.logical_and(at_end, jnp.logical_and(k >= 0, k < TILE_COLS))
        mine = tid(side, k) == tile
        send(jnp.logical_and(ok, jnp.logical_not(mine)), spb.at[pl.ds(8 * jj, 8), 2 * side],
             home_corner.at[r], 37 + jj, 38 + r, panel, tid(side, k))
    send(has_left, spb.at[pl.ds(seam_rows, 8), 0], home_right, 55, 40, panel, tid(r, c - 1))
    send(has_right, spb.at[pl.ds(seam_rows, 8), 2], home_left, 56, 41, panel, tid(r, c + 1))
    send(has_left, spb.at[pl.ds(8, 128), 0], from_right, 57, 42, panel, tid(r, c - 1))
    send(has_right, spb.at[pl.ds(8, 128), 2], from_left, 58, 43, panel, tid(r, c + 1))
    send(yes, spb.at[pl.ds(inner_rows, 8), 1], from_vert, 59, 44, panel, tid(other, c))
    send(has_left, spb.at[pl.ds(inner_rows, 8), 0], from_dr, 60, 45, panel, tid(other, c - 1))
    send(has_right, spb.at[pl.ds(inner_rows, 8), 2], from_dl, 61, 46, panel, tid(other, c + 1))

    @pl.when(is_self)
    def _():
        home_corner[r] = spb[pl.ds(pos, 8), 2 * r]

    first_corner = jnp.logical_or(c <= 15, c == 16)
    second_corner = jnp.logical_or(c >= 16, c == 15)
    arrived(jnp.logical_and(first_corner, tile != 0), home_corner.at[0], 38)
    arrived(jnp.logical_and(second_corner, tile != 2 * TILE_COLS - 1), home_corner.at[1], 39)
    arrived(has_right, home_right, 40)
    arrived(has_left, home_left, 41)
    f32 = jnp.float32
    by_row = cube[pl.ds(seam_rows, 8), 1] + home_left[...].astype(f32) + home_right[...].astype(f32)
    by_col = home_corner[0].astype(f32) + home_corner[1].astype(f32)
    send_b[...] = jnp.where(rowf, by_row, by_col).astype(jnp.bfloat16)
    across_panels(send_b, recv_b, 62, 47)
    turn = turned(recv_b)
    cb_buf[...] = jnp.where(rowf, zero_f, turn).astype(jnp.bfloat16)
    seam_add = jnp.where(rowf, turn, zero_f)
    send(jnp.logical_not(is_self), cb_buf, corner_in.at[pl.ds(8 * (c - 16 * half), 8)], 74,
         59 + c - 16 * half, panel, corner_tile)

    arrived(has_right, from_right, 42)
    arrived(has_left, from_left, 43)
    arrived(yes, from_vert, 44)
    arrived(has_right, from_dr, 45)
    arrived(has_left, from_dl, 46)
    out[...] = cube[pl.ds(8, 128), 1]

    @pl.when(has_right)
    def _():
        out[...] += from_right[...].astype(f32)
        out[pl.ds(120 * other, 8)] += from_dr[...].astype(f32)

    @pl.when(has_left)
    def _():
        out[...] += from_left[...].astype(f32)
        out[pl.ds(120 * other, 8)] += from_dl[...].astype(f32)

    out[pl.ds(120 * other, 8)] += from_vert[...].astype(f32)
    out[pl.ds(120 * r, 8)] += seam_add

    @pl.when(is_self)
    def _():
        corner_in[pl.ds(8 * (c - 16 * half), 8)] = cb_buf[...]

    for j in range(16):
        home = tid(side, 16 * r + j)
        arrived(jnp.logical_and(at_end, home != tile), corner_in.at[pl.ds(8 * j, 8)], 59 + j)

    @pl.when(at_end)
    def _():
        out[...] += corner_in[...].astype(f32)

    out_copy = pltpu.make_async_copy(out, out_hbm, local_sem.at[1])
    out_copy.start()
    for cond, src, dst, slot, rslot, pan, til in sends:
        @pl.when(cond)
        def _():
            remote(src, dst, slot, rslot, pan, til).wait_send()
    out_copy.wait()


def local(residual, inverse, blend_weight, seam_table):
    bf16, f32 = jnp.bfloat16, jnp.float32
    chunk = pltpu.VMEM((8, 8, 128), bf16)
    scratch = [
        pltpu.VMEM((H, 8, 128), f32),
        pltpu.VMEM((NSUB, CELLS, CELLS), bf16),
        pltpu.VMEM((CELLS, 128), f32),
        pltpu.VMEM((144, 3, 8, 128), bf16),
        pltpu.VMEM((144 * 24, 128), f32),
        pltpu.VMEM((144, 3, 8, 128), bf16),
        pltpu.VMEM((H, 8, 128), f32),
        chunk,
        chunk,
        pltpu.VMEM((12, 8, 8, 128), bf16),
        chunk, chunk,
        pltpu.VMEM((64, 128), f32), pltpu.VMEM((64, 128), f32),
        pltpu.VMEM((H, 8, 128), bf16), pltpu.VMEM((H, 8, 128), bf16),
        chunk, chunk, chunk,
        chunk, chunk,
        pltpu.VMEM((2, 8, 8, 128), bf16),
        chunk,
        pltpu.VMEM((12, 8, 8, 128), bf16),
        chunk,
        pltpu.VMEM((H, 8, 128), bf16),
        pltpu.SemaphoreType.DMA((2,)),
        pltpu.SemaphoreType.DMA((NSUB,)),
        pltpu.SemaphoreType.DMA((SEND_COUNT,)),
        pltpu.SemaphoreType.DMA((RECV_COUNT,)),
    ]
    any_space = pl.BlockSpec(memory_space=pl.ANY)
    out = pl.pallas_call(
        kernel,
        out_shape=jax.ShapeDtypeStruct((H, 8, 128), f32),
        in_specs=[pl.BlockSpec(memory_space=pltpu.SMEM), any_space, any_space,
                  pl.BlockSpec(memory_space=pltpu.VMEM)],
        out_specs=any_space,
        scratch_shapes=scratch,
        compiler_params=pltpu.CompilerParams(
            collective_id=0, has_side_effects=True, vmem_limit_bytes=56 * 1024 * 1024),
        name="schwarz",
    )(seam_table, residual[0, 0], inverse[0, 0], blend_weight.reshape(1, CELLS))
    return out[None, None]


def solution(mesh):
    placed = (P("panel", "tile", None, None, None), P("panel", "tile", None, None, None), P(), P())
    return jax.shard_map(
        local,
        mesh=mesh,
        in_specs=placed,
        out_specs=P("panel", "tile", None, None, None),
        check_vma=False,
    )
```

```python
import jax
import jax.numpy as jnp
from jax import lax
from jax.experimental import pallas as pl
from jax.experimental.pallas import tpu as pltpu
from jax.sharding import PartitionSpec as P

PANELS = 4
TILE_COLS = 32
H = 128
LAST = TILE_COLS - 1
NSUB = 16
CELLS = 576
MESH = pl.DeviceIdType.MESH
SENDS = 130
BF16, F32 = jnp.bfloat16, jnp.float32

HALO, HALO_BACK = 0, 5
IN_HOME, CROSS, CROSS_BACK = 10, 18, 21
ROW_GHOST, COL_GHOST = 24, 30
ROW_BACK, COL_BACK = 66, 78
ROW_OWN, COL_OWN = 86, 88
RECVS = 120


def home_of(mu, part):
    z, x = mu % 8, mu // 8
    low = min(z, 7 - z)
    inner = low in (0, 3)
    col = (1 if inner else 0) if z < 4 else (6 if inner else 7)
    return (2 * (low // 2) + part) * 16 + (x ^ part) * 8 + (7 - col if part else col)


def home_at(mu, part):
    z, x = lax.rem(mu, 8), mu // 8
    low = jnp.minimum(z, 7 - z)
    inner = jnp.where(jnp.logical_or(low == 0, low == 3), 1, 0)
    col = jnp.where(z < 4, inner, 7 - inner)
    up = low // 2
    if part:
        return (2 * up + 1) * 16 + (1 - x) * 8 + 7 - col
    return (2 * up) * 16 + x * 8 + col


def kernel(seam, res, inv_hbm, weight, out, inv, ends, wrep, ext, spread, colg, colb, sides, inners, tr, rowg, rowt, own_back, corner_in,
           in_home, cross_out, cross_in, row_out, col_out, row_back, col_back, back_out, back_in,
           xf, yf, zf, rg, from_left, from_right, from_vert, from_dl, from_dr, inv_sem, send_sem, recv_sem):
    panel = lax.axis_index("panel")
    tile = lax.axis_index("tile")
    r = tile // TILE_COLS
    c = lax.rem(tile, TILE_COLS)
    other = 1 - r
    has_left = c > 0
    has_right = c < LAST
    at_end = jnp.logical_or(c == 0, c == LAST)
    side = jnp.where(c == LAST, 1, 0)
    half = c // 16
    seam_rows = 136 * r
    inner_rows = 136 * other
    yes = tile >= 0

    ty, tx, tz = tile // 16, lax.rem(tile // 8, 2), lax.rem(tile, 8)
    part = lax.rem(ty, 2)
    z0 = jnp.where(part == 1, 7 - tz, tz)
    is_home = jnp.logical_or(tz < 2, tz > 5)
    inner = jnp.where(jnp.logical_or(tz == 1, tz == 6), 1, 0)
    up = ty // 2
    low = 2 * up + jnp.where(up == inner, 1, 0)
    mu = 8 * jnp.where(part == 1, 1 - tx, tx) + jnp.where(z0 < 4, low, 7 - low)
    middle = mu == 15

    def tid(row, col):
        return row * TILE_COLS + col

    def chunk_home(k, piece):
        first = k < 16
        m = jnp.where(first, k, LAST - k)
        a, b = home_at(m, 0), home_at(m, 1)
        return jnp.where(first, (a, b)[piece], (b, a)[piece])

    def end_home(j, piece):
        def fixed(k):
            if k < 0 or k > LAST:
                return -1
            m = k if k < 16 else LAST - k
            return home_of(m, piece if k < 16 else 1 - piece)
        return jnp.where(r == 0, fixed(j), fixed(16 + j))

    for n in range(NSUB):
        pltpu.make_async_copy(inv_hbm.at[n], inv.at[n], inv_sem.at[n]).start()

    @pl.when(at_end)
    def _():
        colg[...] = jnp.zeros_like(colg)
        rowg[...] = jnp.zeros_like(rowg)

    @pl.when(is_home)
    def _():
        row_back[...] = jnp.zeros_like(row_back)
        col_back[...] = jnp.zeros_like(col_back)

    barrier = pltpu.get_barrier_semaphore()
    greeted = [jnp.int32(0)]

    def signal(cond, pan, til):
        def now():
            pl.semaphore_signal(barrier, inc=1, device_id=(pan, til), device_id_type=MESH)
        if cond is None:
            now()
        else:
            pl.when(cond)(now)

    def greet(cond, pan, til):
        signal(cond, pan, til)
        greeted[0] = greeted[0] + cond.astype(jnp.int32)

    def both(a, *b):
        for x in b:
            a = jnp.logical_and(a, x)
        return a

    def within(k):
        return jnp.logical_and(k >= 0, k < TILE_COLS)

    served_rows = []
    for slot in range(2):
        for high in range(2):
            k = (LAST - mu) if high else mu
            for b in range(3):
                col = k + 1 - b
                served_rows.append((slot, high, b, tid(slot, col), both(is_home, within(col))))
    served_ends = []
    lowpos, highpos = 8 * mu + 4 * part, 8 * (15 - mu) + 4 * (1 - part)
    for slot in range(2):
        served_ends.append((slot, 0, 0, tid(0, LAST * slot), is_home, 8 + lowpos))
        served_ends.append((slot, 1, 1, tid(1, LAST * slot), is_home, 8 + highpos))
        served_ends.append((slot, 0, 1, tid(1, LAST * slot), both(is_home, middle), 4 * part))
        served_ends.append((slot, 1, 0, tid(0, LAST * slot), both(is_home, middle), 136 + 4 * (1 - part)))
    tile_homes = []
    for b in range(3):
        for piece in range(2):
            k = c + b - 1
            tile_homes.append((b, piece, chunk_home(k, piece), within(k)))
    end_homes = []
    for jj in range(18):
        for piece in range(2):
            home = end_home(jj - 1, piece)
            end_homes.append((jj, piece, home, both(at_end, home >= 0)))

    greet(has_left, panel, tid(r, c - 1))
    greet(has_right, panel, tid(r, c + 1))
    greet(yes, panel, tid(other, c))
    greet(has_left, panel, tid(other, c - 1))
    greet(has_right, panel, tid(other, c + 1))
    for _, _, home, cond in tile_homes:
        greet(both(cond, home != tile), panel, home)

    @pl.when(is_home)
    def _():
        for _, _, _, til, cond in served_rows:
            signal(both(cond, til != tile), panel, til)
        for _, _, _, til, cond, _ in served_ends:
            signal(both(cond, til != tile), panel, til)
        for step in range(1, PANELS):
            signal(None, lax.rem(panel + step, PANELS), tile)

    @pl.when(at_end)
    def _():
        for jj, _, home, cond in end_homes:
            signal(both(cond, home != tile), panel, home)

    for _, _, _, til, cond in served_rows:
        greeted[0] = greeted[0] + both(cond, til != tile).astype(jnp.int32)
    for _, _, _, til, cond, _ in served_ends:
        greeted[0] = greeted[0] + both(cond, til != tile).astype(jnp.int32)
    for _, _, home, cond in end_homes:
        greeted[0] = greeted[0] + both(cond, home != tile).astype(jnp.int32)
    greeted[0] = greeted[0] + jnp.where(is_home, 3, 0)

    ext[8:136, 1] = res[...].astype(BF16)
    for b in range(3):
        ext[pl.ds(seam_rows, 8), b] = jnp.zeros((8, 8, 128), BF16)

    @pl.when(at_end)
    def _():
        for i in range(0, 144, 16):
            ext[i:i + 16, 2 * side] = jnp.zeros((16, 8, 128), BF16)
    xf[...] = res[pl.ds(120 * r, 8)].reshape(64, 128)
    for p in range(8):
        tr[p] = xf[pl.ds(p, 8, stride=8), :].astype(BF16)

    row_type = jnp.where(seam[0, panel, 1] >= 0, 1, 0)
    facts = []
    for slot in range(2):
        edge = 2 * slot + row_type
        facing_panel = jnp.maximum(seam[0, panel, edge], 0)
        facing = lax.rem(edge + 2 + seam[1, panel, edge], 4)
        rev = jnp.where(seam[2, panel, edge] > 0, 1, 0)
        flip = jnp.where((facing >= 2) == (slot == 1), 1, 0)
        pick = jnp.clip(lax.rem(facing_panel - panel + 3, 4), 0, 2)
        facts.append((pick, rev, flip))
    rowf = jnp.full((64, 128), row_type, jnp.int32) == 1
    to_second = [jnp.where(seam[0, panel, 2 + row_type] == lax.rem(panel + step, PANELS), 1, 0)
                 for step in range(1, PANELS)]

    pl.semaphore_wait(barrier, greeted[0])

    def remote(src, dst, slot, rslot, pan, til):
        return pltpu.make_async_remote_copy(
            src_ref=src, dst_ref=dst, send_sem=send_sem.at[slot], recv_sem=recv_sem.at[rslot],
            device_id=(pan, til), device_id_type=MESH)

    used = [0]
    stand_in = {4: tr.at[pl.ds(0, 4)], 8: tr, 128: corner_in, 2: cross_out.at[0]}

    def send(cond, src, dst, rslot, til, pan=None):
        pan = panel if pan is None else pan
        slot = used[0]
        used[0] += 1

        def now():
            remote(src, dst, slot, rslot, pan, til).start()
        if cond is None:
            now()
        else:
            pl.when(cond)(now)
        books[-1][1].append((cond, slot, src.shape[0]))

    def deliver(cond, src, dst, rslot, til):
        send(both(cond, til != tile), src, dst, rslot, til)

        @pl.when(both(cond, til == tile))
        def _():
            dst[...] = src[...]
        _, slot, size = books[-1][1].pop()
        books[-1][1].append(((cond, til), slot, size))

    books = [(None, [])]

    def block(cond, body):
        books.append((cond, []))
        pl.when(cond)(body)
        books.append((None, []))

    def sent():
        def settle(entries):
            for cond, slot, size in entries:
                if isinstance(cond, tuple):
                    cond = both(cond[0], cond[1] != tile)
                ref = stand_in[size]

                def done():
                    remote(ref, ref, slot, 0, panel, tile).wait_send()
                if cond is None:
                    done()
                else:
                    pl.when(cond)(done)
        for cond, entries in books:
            if cond is None:
                settle(entries)
            else:
                pl.when(cond)(lambda: settle(entries))
        books[:] = [(None, [])]

    def arrived(cond, dst, rslot):
        def now():
            remote(dst, dst, 0, rslot, panel, tile).wait_recv()
        if cond is None:
            now()
        else:
            pl.when(cond)(now)

    def ends_in():
        for jj, piece, home, cond in end_homes:
            if 1 <= jj <= 16:
                deliver(yes, ext.at[pl.ds(8 * jj + 4 * piece, 4), 1], in_home.at[0, side, r],
                        IN_HOME + 2 * side + r, home)
    block(at_end, ends_in)
    for b, piece, home, cond in tile_homes:
        if b == 1:
            deliver(cond, tr.at[pl.ds(4 * piece, 4)], in_home.at[1, r, half],
                    IN_HOME + 4 + 2 * r + half, home)
    edge_src = ext.at[pl.ds(128 - 120 * r, 8), 1]
    send(None, edge_src, ext.at[pl.ds(136 * r, 8), 1], HALO, tid(other, c))
    send(has_right, edge_src, ext.at[pl.ds(136 * r, 8), 0], HALO + 1, tid(other, c + 1))
    send(has_left, edge_src, ext.at[pl.ds(136 * r, 8), 2], HALO + 2, tid(other, c - 1))
    mid = ext.at[pl.ds(8, 128), 1]
    send(has_right, mid, ext.at[pl.ds(8, 128), 0], HALO + 3, tid(r, c + 1))
    send(has_left, mid, ext.at[pl.ds(8, 128), 2], HALO + 4, tid(r, c - 1))

    def turned(landed, slot):
        pick, rev, flip = facts[slot]
        yf[...] = landed[pick].astype(F32).reshape(64, 128)
        turn = 1 - 2 * flip
        for high in range(2):
            for i in range(4):
                first = jnp.where(rev == 1, 32 * (1 - high) + 8 * (3 - i), 32 * high + 8 * i) + 7 * flip
                for d in range(8):
                    zf[pl.ds(32 * high + 8 * i + d, 1), :] = yf[pl.ds(first + turn * d, 1), :]
        return zf[0:64, :]

    def cross(landing, source, first_slot):
        def out_of_panel():
            for step in range(1, PANELS):
                send(None, source.at[step - 1], landing.at[3 - step], first_slot + 3 - step, tile,
                     lax.rem(panel + step, PANELS))
        block(is_home, out_of_panel)

    def hand_out(landing, first_slot):
        for i in range(3):
            remote(landing.at[i], landing.at[i], 0, first_slot + i, panel, tile).wait_recv()
        for slot in range(2):
            value = turned(landing, slot)
            blank = jnp.zeros_like(value)
            row_out[slot] = jnp.where(rowf, value, blank).astype(BF16).reshape(2, 4, 8, 128)
            col_out[slot] = jnp.where(rowf, blank, value).astype(BF16).reshape(2, 4, 8, 128)

    for k in range(0, CELLS, 64):
        some = jnp.broadcast_to(weight[pl.ds(k, 64)].reshape(1, 64), (128, 64))
        wrep[pl.ds(k, 64), :] = jnp.transpose(some, (1, 0))
    for n in range(NSUB):
        pltpu.make_async_copy(inv_hbm.at[n], inv.at[n], inv_sem.at[n]).wait()

    @pl.when(at_end)
    def _():
        place = lax.broadcasted_iota(jnp.int32, (CELLS, 192), 0)
        want = lax.broadcasted_iota(jnp.int32, (CELLS, 192), 1)
        want = 24 * lax.div(want, 8) + lax.rem(want, 8) + 16 * side
        choose = jnp.where(place == want, 1.0, 0.0).astype(BF16)

        def gather(n, carry):
            ends[n] = jnp.dot(inv[n], choose, preferred_element_type=F32).astype(BF16)
            return carry
        lax.fori_loop(0, NSUB, gather, 0)

    came_rows = []
    for slot in range(2):
        for high in range(2):
            k = (LAST - mu) if high else mu
            came_rows.append((1, slot, high, tid(slot, k)))
            came_rows.append((0, slot, high, tid(high, LAST * slot)))

    @pl.when(is_home)
    def _():
        for kind, slot, high, til in came_rows:
            arrived(til != tile, in_home.at[kind, slot, high], IN_HOME + 4 * kind + 2 * slot + high)
        for step in range(3):
            cross_out[step] = in_home[row_type, to_second[step]]
    cross(cross_in, cross_out, CROSS)

    spread[...] = jnp.zeros_like(spread)

    @pl.when(is_home)
    def _():
        hand_out(cross_in, CROSS)

    def ghosts_out():
        for slot, high, row, til, cond, at in served_ends:
            deliver(cond, col_out.at[slot, high], colg.at[pl.ds(at, 4)], COL_GHOST + at // 4, til)
        for slot, high, b, til, cond in served_rows:
            piece = (1 - part) if high else part
            deliver(cond, row_out.at[slot, high], rowg.at[pl.ds(8 * b + 4 * piece, 4)], ROW_GHOST + 2 * b + piece, til)
    block(is_home, ghosts_out)

    arrived(None, ext.at[pl.ds(inner_rows, 8), 1], HALO)
    arrived(has_left, ext.at[pl.ds(inner_rows, 8), 0], HALO + 1)
    arrived(has_right, ext.at[pl.ds(inner_rows, 8), 2], HALO + 2)
    arrived(has_left, ext.at[pl.ds(8, 128), 0], HALO + 3)
    arrived(has_right, ext.at[pl.ds(8, 128), 2], HALO + 4)
    flat = ext.reshape(144 * 24, 128)

    def solve(n, carry):
        rows = pl.ds(pl.multiple_of(n * 192, 64), CELLS)
        solved = jnp.dot(inv[n], flat[rows, :], preferred_element_type=F32)
        spread[rows, :] += solved * wrep[...]
        return carry

    lax.fori_loop(0, NSUB, solve, 0)

    end_cells = colg.reshape(144 * 8, 128)

    @pl.when(at_end)
    def _():
        for jj, piece, home, cond in end_homes:
            arrived(both(cond, home != tile), colg.at[pl.ds(8 * jj + 4 * piece, 4)], COL_GHOST + 2 * jj + piece)

        def add(n, carry):
            rows = pl.ds(pl.multiple_of(n * 192, 64), CELLS)
            some = end_cells[pl.ds(pl.multiple_of(n * 64, 64), 192), :]
            spread[rows, :] += jnp.dot(ends[n], some, preferred_element_type=F32) * wrep[...]
            return carry
        lax.fori_loop(0, NSUB, add, 0)

    for b, piece, home, cond in tile_homes:
        arrived(both(cond, home != tile), rowg.at[pl.ds(8 * b + 4 * piece, 4)], ROW_GHOST + 2 * b + piece)
    zf[...] = rowg[...].astype(F32).reshape(192, 128)
    for i in range(8):
        rg[24 * i:24 * i + 24, :] = zf[pl.ds(i, 24, stride=8), :]

    @pl.when(r == 0)
    def _():
        more = jnp.dot(inv[0][:, 0:192], rg[...].astype(BF16), preferred_element_type=F32)
        spread[0:CELLS, :] += more * wrep[...]

    @pl.when(r == 1)
    def _():
        more = jnp.dot(inv[NSUB - 1][:, 384:CELLS], rg[...].astype(BF16), preferred_element_type=F32)
        spread[192 * (NSUB - 1):, :] += more * wrep[...]

    cube = spread.reshape(144, 3, 8, 128)

    def ends_back():
        for i in range(0, 144, 16):
            colb[i:i + 16] = cube[i:i + 16, 2 * side].astype(BF16)
        for jj, piece, home, cond in end_homes:
            high = jnp.where(16 * r + jj - 1 >= 16, 1, 0)
            deliver(cond, colb.at[pl.ds(8 * jj + 4 * piece, 4)], col_back.at[side, high, r],
                    COL_BACK + 4 * side + 2 * high + r, home)
    block(at_end, ends_back)
    for p in range(24):
        rowt[p] = spread[pl.ds(24 * seam_rows + p, 8, stride=24), :].astype(BF16)
    for b, piece, home, cond in tile_homes:
        high = jnp.where(c + b - 1 >= 16, 1, 0)
        deliver(cond, rowt.at[pl.ds(8 * b + 4 * piece, 4)], row_back.at[r, high, b],
                ROW_BACK + 6 * r + 3 * high + b, home)
    for b in range(3):
        inners[b] = cube[pl.ds(inner_rows, 8), b].astype(BF16)
    send(None, inners.at[1], from_vert, HALO_BACK + 2, tid(other, c))
    send(has_left, inners.at[0], from_dr, HALO_BACK + 3, tid(other, c - 1))
    send(has_right, inners.at[2], from_dl, HALO_BACK + 4, tid(other, c + 1))
    for b in range(2):
        for i in range(0, 128, 16):
            sides[b, i:i + 16] = cube[8 + i:24 + i, 2 * b].astype(BF16)
    send(has_left, sides.at[0], from_right, HALO_BACK, tid(r, c - 1))
    send(has_right, sides.at[1], from_left, HALO_BACK + 1, tid(r, c + 1))

    @pl.when(is_home)
    def _():
        for slot, high, b, til, cond in served_rows:
            arrived(both(cond, til != tile), row_back.at[slot, high, b], ROW_BACK + 6 * slot + 3 * high + b)
        for slot, high, row, til, cond, _ in served_ends:
            arrived(both(cond, til != tile), col_back.at[slot, high, row], COL_BACK + 4 * slot + 2 * high + row)
        for slot in range(2):
            for high in range(2):
                by_row = row_back[slot, high, 0].astype(F32) + row_back[slot, high, 1].astype(F32)
                by_row = by_row + row_back[slot, high, 2].astype(F32)
                by_col = col_back[slot, high, 0].astype(F32) + col_back[slot, high, 1].astype(F32)
                mask = jnp.full((4, 8, 128), row_type, jnp.int32) == 1
                in_home[0, slot, high] = jnp.where(mask, by_row, by_col).astype(BF16)
        for step in range(3):
            back_out[step] = in_home[0, to_second[step]]
    cross(back_in, back_out, CROSS_BACK)

    arrived(has_right, from_right, HALO_BACK)
    arrived(has_left, from_left, HALO_BACK + 1)
    arrived(None, from_vert, HALO_BACK + 2)
    arrived(has_left, from_dl, HALO_BACK + 4)
    arrived(has_right, from_dr, HALO_BACK + 3)
    out[...] = cube[pl.ds(8, 128), 1]

    @pl.when(has_right)
    def _():
        out[...] += from_right[...].astype(F32)
        out[pl.ds(120 * other, 8)] += from_dr[...].astype(F32)

    @pl.when(has_left)
    def _():
        out[...] += from_left[...].astype(F32)
        out[pl.ds(120 * other, 8)] += from_dl[...].astype(F32)

    out[pl.ds(120 * other, 8)] += from_vert[...].astype(F32)

    sent()

    @pl.when(is_home)
    def _():
        hand_out(back_in, CROSS_BACK)

    def sums_out():
        for slot, high, row, til, cond, at in served_ends:
            if row == high:
                pos = highpos if high else lowpos
                deliver(yes, col_out.at[slot, high], corner_in.at[pl.ds(pos, 4)], COL_OWN + pos // 4, til)
        for slot, high, b, til, cond in served_rows:
            if b == 1:
                piece = (1 - part) if high else part
                deliver(yes, row_out.at[slot, high], own_back.at[pl.ds(4 * piece, 4)], ROW_OWN + piece, til)
    block(is_home, sums_out)
    for b, piece, home, cond in tile_homes:
        if b == 1:
            arrived(both(cond, home != tile), own_back.at[pl.ds(4 * piece, 4)], ROW_OWN + piece)
    xf[...] = own_back[...].astype(F32).reshape(64, 128)
    for i in range(8):
        out[120 * r + i] += xf[pl.ds(i, 8, stride=8), :]

    @pl.when(at_end)
    def _():
        for jj, piece, home, cond in end_homes:
            if 1 <= jj <= 16:
                arrived(home != tile, corner_in.at[pl.ds(8 * (jj - 1) + 4 * piece, 4)],
                        COL_OWN + 2 * (jj - 1) + piece)
        out[...] += corner_in[...].astype(F32)
    sent()


def local(residual, inverse, blend_weight, seam_table):
    def vmem(*shape, dtype=BF16):
        return pltpu.VMEM(shape, dtype)
    unit = (4, 8, 128)
    scratch = [
        vmem(NSUB, CELLS, CELLS),
        vmem(NSUB, CELLS, 192),
        vmem(CELLS, 128, dtype=F32),
        vmem(144, 3, 8, 128),
        vmem(144 * 24, 128, dtype=F32),
        vmem(144, 8, 128), vmem(144, 8, 128),
        vmem(2, H, 8, 128), vmem(3, 8, 8, 128),
        vmem(8, 8, 128),
        vmem(24, 8, 128),
        vmem(24, 8, 128),
        vmem(8, 8, 128),
        vmem(H, 8, 128),
        vmem(2, 2, 2, *unit),
        vmem(3, 2, *unit), vmem(3, 2, *unit),
        vmem(2, 2, *unit), vmem(2, 2, *unit),
        vmem(2, 2, 3, *unit),
        vmem(2, 2, 2, *unit),
        vmem(3, 2, *unit), vmem(3, 2, *unit),
        vmem(64, 128, dtype=F32),
        vmem(64, 128, dtype=F32),
        vmem(192, 128, dtype=F32),
        vmem(192, 128, dtype=F32),
        vmem(H, 8, 128), vmem(H, 8, 128),
        vmem(8, 8, 128), vmem(8, 8, 128), vmem(8, 8, 128),
        pltpu.SemaphoreType.DMA((NSUB,)),
        pltpu.SemaphoreType.DMA((SENDS,)),
        pltpu.SemaphoreType.DMA((RECVS,)),
    ]
    in_vmem = pl.BlockSpec(memory_space=pltpu.VMEM)
    out = pl.pallas_call(
        kernel,
        out_shape=jax.ShapeDtypeStruct((H, 8, 128), F32),
        in_specs=[pl.BlockSpec(memory_space=pltpu.SMEM), in_vmem, pl.BlockSpec(memory_space=pltpu.HBM), in_vmem],
        out_specs=in_vmem,
        scratch_shapes=scratch,
        compiler_params=pltpu.CompilerParams(
            collective_id=0, has_side_effects=True, vmem_limit_bytes=46 * 1024 * 1024),
        name="schwarz",
    )(jnp.transpose(seam_table, (2, 0, 1)), residual[0, 0], inverse[0, 0], blend_weight)
    return out[None, None]


def solution(mesh):
    placed = (P("panel", "tile", None, None, None), P("panel", "tile", None, None, None), P(), P())
    return jax.shard_map(
        local,
        mesh=mesh,
        in_specs=placed,
        out_specs=P("panel", "tile", None, None, None),
        check_vma=False,
    )
```

```python
import jax
import jax.numpy as jnp
from jax import lax
from jax.experimental import pallas as pl
from jax.experimental.pallas import tpu as pltpu
from jax.sharding import PartitionSpec as P

PANELS = 4
TILE_COLS = 32
H = 128
LAST = TILE_COLS - 1
NSUB = 16
CELLS = 576
MESH = pl.DeviceIdType.MESH
SENDS = 130
BF16, F32 = jnp.bfloat16, jnp.float32

HALO, HALO_BACK = 0, 5
IN_HOME, CROSS, CROSS_BACK = 10, 18, 21
ROW_GHOST, COL_GHOST = 24, 30
ROW_BACK, COL_BACK = 66, 78
ROW_OWN, COL_OWN = 86, 88
RECVS = 120


HOMES = ((7, 8), (41, 22), (9, 10), (2, 5), (26, 29), (14, 17), (15, 16), (39, 56),
         (40, 55), (47, 33), (1, 30), (21, 34), (37, 42), (6, 25), (38, 48), (24, 23))


def home_of(k, piece):
    if k < 0 or k > LAST:
        return -1
    return HOMES[k][piece] if k < 16 else HOMES[LAST - k][1 - piece]


def kernel(seam_hbm, res_hbm, inv_hbm, weight_hbm, out, seam, res, weight, inv, ends, wrep, ext, spread, colg, colb, sides, inners, tr, rowg, rowt, own_back, corner_in,
           in_home, cross_out, cross_in, row_out, col_out, row_back, col_back, back_out, back_in,
           xf, yf, zf, rg, from_left, from_right, from_vert, from_dl, from_dr, in_sem, inv_sem, send_sem, recv_sem):
    panel = lax.axis_index("panel")
    tile = lax.axis_index("tile")
    r = tile // TILE_COLS
    c = lax.rem(tile, TILE_COLS)
    other = 1 - r
    has_left = c > 0
    has_right = c < LAST
    at_end = jnp.logical_or(c == 0, c == LAST)
    side = jnp.where(c == LAST, 1, 0)
    half = c // 16
    seam_rows = 136 * r
    inner_rows = 136 * other
    yes = tile >= 0

    role = jnp.int32(-1)
    for m in range(16):
        for p in range(2):
            role = jnp.where(tile == HOMES[m][p], 2 * m + p, role)
    is_home = role >= 0
    role = jnp.maximum(role, 0)
    mu, part = role // 2, lax.rem(role, 2)
    middle = mu == 15

    def tid(row, col):
        return row * TILE_COLS + col

    def end_home(j, piece):
        return jnp.where(r == 0, home_of(j, piece), home_of(16 + j, piece))

    inputs = [pltpu.make_async_copy(a, b, in_sem.at[i])
              for i, (a, b) in enumerate(((res_hbm, res), (seam_hbm, seam), (weight_hbm, weight)))]
    for copy in inputs:
        copy.start()
    for n in range(NSUB):
        pltpu.make_async_copy(inv_hbm.at[n], inv.at[n], inv_sem.at[n]).start()

    @pl.when(at_end)
    def _():
        colg[...] = jnp.zeros_like(colg)
        rowg[...] = jnp.zeros_like(rowg)

    @pl.when(is_home)
    def _():
        row_back[...] = jnp.zeros_like(row_back)
        col_back[...] = jnp.zeros_like(col_back)

    barrier = pltpu.get_barrier_semaphore()
    greeted = [jnp.int32(0)]

    def signal(cond, pan, til):
        def now():
            pl.semaphore_signal(barrier, inc=1, device_id=(pan, til), device_id_type=MESH)
        if cond is None:
            now()
        else:
            pl.when(cond)(now)

    def greet(cond, pan, til):
        signal(cond, pan, til)
        greeted[0] = greeted[0] + cond.astype(jnp.int32)

    def both(a, *b):
        for x in b:
            a = jnp.logical_and(a, x)
        return a

    def within(k):
        return jnp.logical_and(k >= 0, k < TILE_COLS)

    served_rows = []
    for slot in range(2):
        for high in range(2):
            k = (LAST - mu) if high else mu
            for b in range(3):
                col = k + 1 - b
                served_rows.append((slot, high, b, tid(slot, col), both(is_home, within(col))))
    served_ends = []
    lowpos, highpos = 8 * mu + 4 * part, 8 * (15 - mu) + 4 * (1 - part)
    for slot in range(2):
        served_ends.append((slot, 0, 0, tid(0, LAST * slot), is_home, 8 + lowpos))
        served_ends.append((slot, 1, 1, tid(1, LAST * slot), is_home, 8 + highpos))
        served_ends.append((slot, 0, 1, tid(1, LAST * slot), both(is_home, middle), 4 * part))
        served_ends.append((slot, 1, 0, tid(0, LAST * slot), both(is_home, middle), 136 + 4 * (1 - part)))
    tile_homes = []
    for b in range(3):
        for piece in range(2):
            home = jnp.int32(-1)
            for i in range(TILE_COLS):
                home = jnp.where(c == i, home_of(i + b - 1, piece), home)
            tile_homes.append((b, piece, home, within(c + b - 1)))
    end_homes = []
    for jj in range(18):
        for piece in range(2):
            home = end_home(jj - 1, piece)
            end_homes.append((jj, piece, home, both(at_end, home >= 0)))

    greet(has_left, panel, tid(r, c - 1))
    greet(has_right, panel, tid(r, c + 1))
    greet(yes, panel, tid(other, c))
    greet(has_left, panel, tid(other, c - 1))
    greet(has_right, panel, tid(other, c + 1))
    for _, _, home, cond in tile_homes:
        greet(both(cond, home != tile), panel, home)

    @pl.when(is_home)
    def _():
        for _, _, _, til, cond in served_rows:
            signal(both(cond, til != tile), panel, til)
        for _, _, _, til, cond, _ in served_ends:
            signal(both(cond, til != tile), panel, til)
        for step in range(1, PANELS):
            signal(None, lax.rem(panel + step, PANELS), tile)

    @pl.when(at_end)
    def _():
        for jj, _, home, cond in end_homes:
            signal(both(cond, home != tile), panel, home)

    for _, _, _, til, cond in served_rows:
        greeted[0] = greeted[0] + both(cond, til != tile).astype(jnp.int32)
    for _, _, _, til, cond, _ in served_ends:
        greeted[0] = greeted[0] + both(cond, til != tile).astype(jnp.int32)
    for _, _, home, cond in end_homes:
        greeted[0] = greeted[0] + both(cond, home != tile).astype(jnp.int32)
    greeted[0] = greeted[0] + jnp.where(is_home, 3, 0)

    for copy in inputs:
        copy.wait()
    ext[8:136, 1] = res[...].astype(BF16)
    for b in range(3):
        ext[pl.ds(seam_rows, 8), b] = jnp.zeros((8, 8, 128), BF16)

    @pl.when(at_end)
    def _():
        for i in range(0, 144, 16):
            ext[i:i + 16, 2 * side] = jnp.zeros((16, 8, 128), BF16)
    xf[...] = res[pl.ds(120 * r, 8)].reshape(64, 128)
    for p in range(8):
        tr[p] = xf[pl.ds(p, 8, stride=8), :].astype(BF16)

    row_type = jnp.where(seam[0, panel, 1] >= 0, 1, 0)
    facts = []
    for slot in range(2):
        edge = 2 * slot + row_type
        facing_panel = jnp.maximum(seam[0, panel, edge], 0)
        facing = lax.rem(edge + 2 + seam[1, panel, edge], 4)
        rev = jnp.where(seam[2, panel, edge] > 0, 1, 0)
        flip = jnp.where((facing >= 2) == (slot == 1), 1, 0)
        pick = jnp.clip(lax.rem(facing_panel - panel + 3, 4), 0, 2)
        facts.append((pick, rev, flip))
    rowf = jnp.full((64, 128), row_type, jnp.int32) == 1
    to_second = [jnp.where(seam[0, panel, 2 + row_type] == lax.rem(panel + step, PANELS), 1, 0)
                 for step in range(1, PANELS)]

    pl.semaphore_wait(barrier, greeted[0])

    def remote(src, dst, slot, rslot, pan, til):
        return pltpu.make_async_remote_copy(
            src_ref=src, dst_ref=dst, send_sem=send_sem.at[slot], recv_sem=recv_sem.at[rslot],
            device_id=(pan, til), device_id_type=MESH)

    used = [0]
    stand_in = {4: tr.at[pl.ds(0, 4)], 8: tr, 128: corner_in, 2: cross_out.at[0]}

    def send(cond, src, dst, rslot, til, pan=None):
        pan = panel if pan is None else pan
        slot = used[0]
        used[0] += 1

        def now():
            remote(src, dst, slot, rslot, pan, til).start()
        if cond is None:
            now()
        else:
            pl.when(cond)(now)
        books[-1][1].append((cond, slot, src.shape[0]))

    def deliver(cond, src, dst, rslot, til):
        send(both(cond, til != tile), src, dst, rslot, til)

        @pl.when(both(cond, til == tile))
        def _():
            dst[...] = src[...]
        _, slot, size = books[-1][1].pop()
        books[-1][1].append(((cond, til), slot, size))

    books = [(None, [])]

    def block(cond, body):
        books.append((cond, []))
        pl.when(cond)(body)
        books.append((None, []))

    def sent():
        def settle(entries):
            for cond, slot, size in entries:
                if isinstance(cond, tuple):
                    cond = both(cond[0], cond[1] != tile)
                ref = stand_in[size]

                def done():
                    remote(ref, ref, slot, 0, panel, tile).wait_send()
                if cond is None:
                    done()
                else:
                    pl.when(cond)(done)
        for cond, entries in books:
            if cond is None:
                settle(entries)
            else:
                pl.when(cond)(lambda: settle(entries))
        books[:] = [(None, [])]

    def arrived(cond, dst, rslot):
        def now():
            remote(dst, dst, 0, rslot, panel, tile).wait_recv()
        if cond is None:
            now()
        else:
            pl.when(cond)(now)

    def ends_in():
        for jj, piece, home, cond in end_homes:
            if 1 <= jj <= 16:
                deliver(yes, ext.at[pl.ds(8 * jj + 4 * piece, 4), 1], in_home.at[0, side, r],
                        IN_HOME + 2 * side + r, home)
    block(at_end, ends_in)
    for b, piece, home, cond in tile_homes:
        if b == 1:
            deliver(cond, tr.at[pl.ds(4 * piece, 4)], in_home.at[1, r, half],
                    IN_HOME + 4 + 2 * r + half, home)
    edge_src = ext.at[pl.ds(128 - 120 * r, 8), 1]
    send(None, edge_src, ext.at[pl.ds(136 * r, 8), 1], HALO, tid(other, c))
    send(has_right, edge_src, ext.at[pl.ds(136 * r, 8), 0], HALO + 1, tid(other, c + 1))
    send(has_left, edge_src, ext.at[pl.ds(136 * r, 8), 2], HALO + 2, tid(other, c - 1))
    mid = ext.at[pl.ds(8, 128), 1]
    send(has_right, mid, ext.at[pl.ds(8, 128), 0], HALO + 3, tid(r, c + 1))
    send(has_left, mid, ext.at[pl.ds(8, 128), 2], HALO + 4, tid(r, c - 1))

    def turned(landed, slot):
        pick, rev, flip = facts[slot]
        yf[...] = landed[pick].astype(F32).reshape(64, 128)
        turn = 1 - 2 * flip
        for high in range(2):
            for i in range(4):
                first = jnp.where(rev == 1, 32 * (1 - high) + 8 * (3 - i), 32 * high + 8 * i) + 7 * flip
                for d in range(8):
                    zf[pl.ds(32 * high + 8 * i + d, 1), :] = yf[pl.ds(first + turn * d, 1), :]
        return zf[0:64, :]

    def cross(landing, source, first_slot):
        def out_of_panel():
            for step in range(1, PANELS):
                send(None, source.at[step - 1], landing.at[3 - step], first_slot + 3 - step, tile,
                     lax.rem(panel + step, PANELS))
        block(is_home, out_of_panel)

    def hand_out(landing, first_slot):
        for i in range(3):
            remote(landing.at[i], landing.at[i], 0, first_slot + i, panel, tile).wait_recv()
        for slot in range(2):
            value = turned(landing, slot)
            blank = jnp.zeros_like(value)
            row_out[slot] = jnp.where(rowf, value, blank).astype(BF16).reshape(2, 4, 8, 128)
            col_out[slot] = jnp.where(rowf, blank, value).astype(BF16).reshape(2, 4, 8, 128)

    for k in range(0, CELLS, 64):
        some = jnp.broadcast_to(weight[pl.ds(k, 64)].reshape(1, 64), (128, 64))
        wrep[pl.ds(k, 64), :] = jnp.transpose(some, (1, 0))
    for n in range(NSUB):
        pltpu.make_async_copy(inv_hbm.at[n], inv.at[n], inv_sem.at[n]).wait()

    @pl.when(at_end)
    def _():
        place = lax.broadcasted_iota(jnp.int32, (CELLS, 192), 0)
        want = lax.broadcasted_iota(jnp.int32, (CELLS, 192), 1)
        want = 24 * lax.div(want, 8) + lax.rem(want, 8) + 16 * side
        choose = jnp.where(place == want, 1.0, 0.0).astype(BF16)

        def gather(n, carry):
            ends[n] = jnp.dot(inv[n], choose, preferred_element_type=F32).astype(BF16)
            return carry
        lax.fori_loop(0, NSUB, gather, 0)

    came_rows = []
    for slot in range(2):
        for high in range(2):
            k = (LAST - mu) if high else mu
            came_rows.append((1, slot, high, tid(slot, k)))
            came_rows.append((0, slot, high, tid(high, LAST * slot)))

    @pl.when(is_home)
    def _():
        for kind, slot, high, til in came_rows:
            arrived(til != tile, in_home.at[kind, slot, high], IN_HOME + 4 * kind + 2 * slot + high)
        for step in range(3):
            cross_out[step] = in_home[row_type, to_second[step]]
    cross(cross_in, cross_out, CROSS)

    spread[...] = jnp.zeros_like(spread)

    @pl.when(is_home)
    def _():
        hand_out(cross_in, CROSS)

    def ghosts_out():
        for slot, high, row, til, cond, at in served_ends:
            deliver(cond, col_out.at[slot, high], colg.at[pl.ds(at, 4)], COL_GHOST + at // 4, til)
        for slot, high, b, til, cond in served_rows:
            piece = (1 - part) if high else part
            deliver(cond, row_out.at[slot, high], rowg.at[pl.ds(8 * b + 4 * piece, 4)], ROW_GHOST + 2 * b + piece, til)
    block(is_home, ghosts_out)

    arrived(None, ext.at[pl.ds(inner_rows, 8), 1], HALO)
    arrived(has_left, ext.at[pl.ds(inner_rows, 8), 0], HALO + 1)
    arrived(has_right, ext.at[pl.ds(inner_rows, 8), 2], HALO + 2)
    arrived(has_left, ext.at[pl.ds(8, 128), 0], HALO + 3)
    arrived(has_right, ext.at[pl.ds(8, 128), 2], HALO + 4)
    flat = ext.reshape(144 * 24, 128)

    def solve(n, carry):
        rows = pl.ds(pl.multiple_of(n * 192, 64), CELLS)
        solved = jnp.dot(inv[n], flat[rows, :], preferred_element_type=F32)
        spread[rows, :] += solved * wrep[...]
        return carry

    lax.fori_loop(0, NSUB, solve, 0)

    end_cells = colg.reshape(144 * 8, 128)

    @pl.when(at_end)
    def _():
        for jj, piece, home, cond in end_homes:
            arrived(both(cond, home != tile), colg.at[pl.ds(8 * jj + 4 * piece, 4)], COL_GHOST + 2 * jj + piece)

        def add(n, carry):
            rows = pl.ds(pl.multiple_of(n * 192, 64), CELLS)
            some = end_cells[pl.ds(pl.multiple_of(n * 64, 64), 192), :]
            spread[rows, :] += jnp.dot(ends[n], some, preferred_element_type=F32) * wrep[...]
            return carry
        lax.fori_loop(0, NSUB, add, 0)

    for b, piece, home, cond in tile_homes:
        arrived(both(cond, home != tile), rowg.at[pl.ds(8 * b + 4 * piece, 4)], ROW_GHOST + 2 * b + piece)
    zf[...] = rowg[...].astype(F32).reshape(192, 128)
    for i in range(8):
        rg[24 * i:24 * i + 24, :] = zf[pl.ds(i, 24, stride=8), :]

    @pl.when(r == 0)
    def _():
        more = jnp.dot(inv[0][:, 0:192], rg[...].astype(BF16), preferred_element_type=F32)
        spread[0:CELLS, :] += more * wrep[...]

    @pl.when(r == 1)
    def _():
        more = jnp.dot(inv[NSUB - 1][:, 384:CELLS], rg[...].astype(BF16), preferred_element_type=F32)
        spread[192 * (NSUB - 1):, :] += more * wrep[...]

    cube = spread.reshape(144, 3, 8, 128)

    def ends_back():
        for i in range(0, 144, 16):
            colb[i:i + 16] = cube[i:i + 16, 2 * side].astype(BF16)
        for jj, piece, home, cond in end_homes:
            high = jnp.where(16 * r + jj - 1 >= 16, 1, 0)
            deliver(cond, colb.at[pl.ds(8 * jj + 4 * piece, 4)], col_back.at[side, high, r],
                    COL_BACK + 4 * side + 2 * high + r, home)
    block(at_end, ends_back)
    for p in range(24):
        rowt[p] = spread[pl.ds(24 * seam_rows + p, 8, stride=24), :].astype(BF16)
    for b, piece, home, cond in tile_homes:
        high = jnp.where(c + b - 1 >= 16, 1, 0)
        deliver(cond, rowt.at[pl.ds(8 * b + 4 * piece, 4)], row_back.at[r, high, b],
                ROW_BACK + 6 * r + 3 * high + b, home)
    for b in range(3):
        inners[b] = cube[pl.ds(inner_rows, 8), b].astype(BF16)
    send(None, inners.at[1], from_vert, HALO_BACK + 2, tid(other, c))
    send(has_left, inners.at[0], from_dr, HALO_BACK + 3, tid(other, c - 1))
    send(has_right, inners.at[2], from_dl, HALO_BACK + 4, tid(other, c + 1))
    for b in range(2):
        for i in range(0, 128, 16):
            sides[b, i:i + 16] = cube[8 + i:24 + i, 2 * b].astype(BF16)
    send(has_left, sides.at[0], from_right, HALO_BACK, tid(r, c - 1))
    send(has_right, sides.at[1], from_left, HALO_BACK + 1, tid(r, c + 1))

    @pl.when(is_home)
    def _():
        for slot, high, b, til, cond in served_rows:
            arrived(both(cond, til != tile), row_back.at[slot, high, b], ROW_BACK + 6 * slot + 3 * high + b)
        for slot, high, row, til, cond, _ in served_ends:
            arrived(both(cond, til != tile), col_back.at[slot, high, row], COL_BACK + 4 * slot + 2 * high + row)
        for slot in range(2):
            for high in range(2):
                by_row = row_back[slot, high, 0].astype(F32) + row_back[slot, high, 1].astype(F32)
                by_row = by_row + row_back[slot, high, 2].astype(F32)
                by_col = col_back[slot, high, 0].astype(F32) + col_back[slot, high, 1].astype(F32)
                mask = jnp.full((4, 8, 128), row_type, jnp.int32) == 1
                in_home[0, slot, high] = jnp.where(mask, by_row, by_col).astype(BF16)
        for step in range(3):
            back_out[step] = in_home[0, to_second[step]]
    cross(back_in, back_out, CROSS_BACK)

    arrived(has_right, from_right, HALO_BACK)
    arrived(has_left, from_left, HALO_BACK + 1)
    arrived(None, from_vert, HALO_BACK + 2)
    arrived(has_left, from_dl, HALO_BACK + 4)
    arrived(has_right, from_dr, HALO_BACK + 3)
    out[...] = cube[pl.ds(8, 128), 1]

    @pl.when(has_right)
    def _():
        out[...] += from_right[...].astype(F32)
        out[pl.ds(120 * other, 8)] += from_dr[...].astype(F32)

    @pl.when(has_left)
    def _():
        out[...] += from_left[...].astype(F32)
        out[pl.ds(120 * other, 8)] += from_dl[...].astype(F32)

    out[pl.ds(120 * other, 8)] += from_vert[...].astype(F32)

    sent()

    @pl.when(is_home)
    def _():
        hand_out(back_in, CROSS_BACK)

    def sums_out():
        for slot, high, row, til, cond, at in served_ends:
            if row == high:
                pos = highpos if high else lowpos
                deliver(yes, col_out.at[slot, high], corner_in.at[pl.ds(pos, 4)], COL_OWN + pos // 4, til)
        for slot, high, b, til, cond in served_rows:
            if b == 1:
                piece = (1 - part) if high else part
                deliver(yes, row_out.at[slot, high], own_back.at[pl.ds(4 * piece, 4)], ROW_OWN + piece, til)
    block(is_home, sums_out)
    for b, piece, home, cond in tile_homes:
        if b == 1:
            arrived(both(cond, home != tile), own_back.at[pl.ds(4 * piece, 4)], ROW_OWN + piece)
    xf[...] = own_back[...].astype(F32).reshape(64, 128)
    for i in range(8):
        out[120 * r + i] += xf[pl.ds(i, 8, stride=8), :]

    @pl.when(at_end)
    def _():
        for jj, piece, home, cond in end_homes:
            if 1 <= jj <= 16:
                arrived(home != tile, corner_in.at[pl.ds(8 * (jj - 1) + 4 * piece, 4)],
                        COL_OWN + 2 * (jj - 1) + piece)
        out[...] += corner_in[...].astype(F32)
    sent()


def local(residual, inverse, blend_weight, seam_table):
    def vmem(*shape, dtype=BF16):
        return pltpu.VMEM(shape, dtype)
    unit = (4, 8, 128)
    scratch = [
        pltpu.SMEM((3, PANELS, 4), jnp.int32),
        vmem(H, 8, 128, dtype=F32),
        vmem(CELLS, dtype=F32),
        vmem(NSUB, CELLS, CELLS),
        vmem(NSUB, CELLS, 192),
        vmem(CELLS, 128, dtype=F32),
        vmem(144, 3, 8, 128),
        vmem(144 * 24, 128, dtype=F32),
        vmem(144, 8, 128), vmem(144, 8, 128),
        vmem(2, H, 8, 128), vmem(3, 8, 8, 128),
        vmem(8, 8, 128),
        vmem(24, 8, 128),
        vmem(24, 8, 128),
        vmem(8, 8, 128),
        vmem(H, 8, 128),
        vmem(2, 2, 2, *unit),
        vmem(3, 2, *unit), vmem(3, 2, *unit),
        vmem(2, 2, *unit), vmem(2, 2, *unit),
        vmem(2, 2, 3, *unit),
        vmem(2, 2, 2, *unit),
        vmem(3, 2, *unit), vmem(3, 2, *unit),
        vmem(64, 128, dtype=F32),
        vmem(64, 128, dtype=F32),
        vmem(192, 128, dtype=F32),
        vmem(192, 128, dtype=F32),
        vmem(H, 8, 128), vmem(H, 8, 128),
        vmem(8, 8, 128), vmem(8, 8, 128), vmem(8, 8, 128),
        pltpu.SemaphoreType.DMA((3,)),
        pltpu.SemaphoreType.DMA((NSUB,)),
        pltpu.SemaphoreType.DMA((SENDS,)),
        pltpu.SemaphoreType.DMA((RECVS,)),
    ]
    given = (jnp.transpose(seam_table, (2, 0, 1)), residual[0, 0], inverse[0, 0], blend_weight)
    out = pl.pallas_call(
        kernel,
        out_shape=jax.ShapeDtypeStruct((H, 8, 128), F32),
        in_specs=[pl.BlockSpec(memory_space=pltpu.HBM)] * 4,
        out_specs=pl.BlockSpec(memory_space=pltpu.VMEM),
        scratch_shapes=scratch,
        compiler_params=pltpu.CompilerParams(
            collective_id=0, has_side_effects=True, vmem_limit_bytes=46 * 1024 * 1024),
        name="schwarz",
    )(*[pltpu.with_memory_space_constraint(a, pltpu.HBM) for a in given])
    return out[None, None]


def solution(mesh):
    placed = (P("panel", "tile", None, None, None), P("panel", "tile", None, None, None), P(), P())
    return jax.shard_map(
        local,
        mesh=mesh,
        in_specs=placed,
        out_specs=P("panel", "tile", None, None, None),
        check_vma=False,
    )
```

```python
import jax
import jax.numpy as jnp
from jax import lax
from jax.experimental import pallas as pl
from jax.experimental.pallas import tpu as pltpu
from jax.sharding import PartitionSpec as P

PANELS = 4
TILE_COLS = 32
H = 128
LAST = TILE_COLS - 1
NSUB = 16
CELLS = 576
MESH = pl.DeviceIdType.MESH
SENDS = 140
FIRST = 7
BF16, F32 = jnp.bfloat16, jnp.float32

HALO, HALO_BACK = 0, 5
IN_HOME, CROSS, CROSS_BACK = 10, 18, 21
ROW_GHOST, COL_GHOST = 24, 30
ROW_BACK, COL_BACK = 66, 78
ROW_OWN, COL_OWN = 86, 88
LATE_ROWS = 120
HALO_REST = 122
RECVS = 124


HOMES = ((7, 8), (41, 22), (9, 10), (2, 5), (26, 29), (14, 17), (15, 16), (39, 56),
         (40, 55), (47, 33), (1, 30), (21, 34), (37, 42), (6, 25), (38, 48), (24, 23))


def home_of(k, piece):
    if k < 0 or k > LAST:
        return -1
    return HOMES[k][piece] if k < 16 else HOMES[LAST - k][1 - piece]


def kernel(seam_hbm, res_hbm, inv_hbm, weight_hbm, out, seam, res, weight, inv, ends, facing_ends, wide, colsum, wrep, ext, spread, colg, colb, sides, inners, tr, rowg, rowt, own_back, corner_in,
           in_home, cross_out, cross_in, row_out, col_out, row_back, col_back, back_out, back_in,
           xf, yf, zf, rg, from_left, from_right, from_vert, from_dl, from_dr, in_sem, inv_sem, send_sem, recv_sem):
    panel = lax.axis_index("panel")
    tile = lax.axis_index("tile")
    r = tile // TILE_COLS
    c = lax.rem(tile, TILE_COLS)
    other = 1 - r
    has_left = c > 0
    has_right = c < LAST
    at_end = jnp.logical_or(c == 0, c == LAST)
    side = jnp.where(c == LAST, 1, 0)
    half = c // 16
    seam_rows = 136 * r
    inner_rows = 136 * other
    yes = tile >= 0

    role = jnp.int32(-1)
    for m in range(16):
        for p in range(2):
            role = jnp.where(tile == HOMES[m][p], 2 * m + p, role)
    is_home = role >= 0
    role = jnp.maximum(role, 0)
    mu, part = role // 2, lax.rem(role, 2)
    middle = mu == 15

    def tid(row, col):
        return row * TILE_COLS + col

    def end_home(j, piece):
        return jnp.where(r == 0, home_of(j, piece), home_of(16 + j, piece))

    inputs = [pltpu.make_async_copy(a, b, in_sem.at[i])
              for i, (a, b) in enumerate(((res_hbm, res), (seam_hbm, seam), (weight_hbm, weight)))]
    for copy in inputs:
        copy.start()
    for n in range(NSUB):
        pltpu.make_async_copy(inv_hbm.at[n], inv.at[n], inv_sem.at[n]).start()

    @pl.when(at_end)
    def _():
        colg[...] = jnp.zeros_like(colg)
        rowg[...] = jnp.zeros_like(rowg)

    @pl.when(is_home)
    def _():
        row_back[...] = jnp.zeros_like(row_back)
        col_back[...] = jnp.zeros_like(col_back)

    barrier = pltpu.get_barrier_semaphore()
    greeted = [jnp.int32(0)]

    def signal(cond, pan, til):
        def now():
            pl.semaphore_signal(barrier, inc=1, device_id=(pan, til), device_id_type=MESH)
        if cond is None:
            now()
        else:
            pl.when(cond)(now)

    def greet(cond, pan, til):
        signal(cond, pan, til)
        greeted[0] = greeted[0] + cond.astype(jnp.int32)

    def both(a, *b):
        for x in b:
            a = jnp.logical_and(a, x)
        return a

    def within(k):
        return jnp.logical_and(k >= 0, k < TILE_COLS)

    served_rows = []
    for slot in range(2):
        for high in range(2):
            k = (LAST - mu) if high else mu
            for b in range(3):
                col = k + 1 - b
                served_rows.append((slot, high, b, tid(slot, col), both(is_home, within(col))))
    served_ends = []
    lowpos, highpos = 8 * mu + 4 * part, 8 * (15 - mu) + 4 * (1 - part)
    for slot in range(2):
        served_ends.append((slot, 0, 0, tid(0, LAST * slot), is_home, 8 + lowpos))
        served_ends.append((slot, 1, 1, tid(1, LAST * slot), is_home, 8 + highpos))
        served_ends.append((slot, 0, 1, tid(1, LAST * slot), both(is_home, middle), 4 * part))
        served_ends.append((slot, 1, 0, tid(0, LAST * slot), both(is_home, middle), 136 + 4 * (1 - part)))
    tile_homes = []
    for b in range(3):
        for piece in range(2):
            home = jnp.int32(-1)
            for i in range(TILE_COLS):
                home = jnp.where(c == i, home_of(i + b - 1, piece), home)
            tile_homes.append((b, piece, home, within(c + b - 1)))
    end_homes = []
    for jj in range(18):
        for piece in range(2):
            home = end_home(jj - 1, piece)
            end_homes.append((jj, piece, home, both(at_end, home >= 0)))

    greet(has_left, panel, tid(r, c - 1))
    greet(has_right, panel, tid(r, c + 1))
    greet(yes, panel, tid(other, c))
    greet(has_left, panel, tid(other, c - 1))
    greet(has_right, panel, tid(other, c + 1))
    for _, _, home, cond in tile_homes:
        greet(both(cond, home != tile), panel, home)

    @pl.when(is_home)
    def _():
        for _, _, _, til, cond in served_rows:
            signal(both(cond, til != tile), panel, til)
        for _, _, _, til, cond, _ in served_ends:
            signal(both(cond, til != tile), panel, til)
        for step in range(1, PANELS):
            signal(None, lax.rem(panel + step, PANELS), tile)

    @pl.when(at_end)
    def _():
        for jj, _, home, cond in end_homes:
            signal(both(cond, home != tile), panel, home)

    for _, _, _, til, cond in served_rows:
        greeted[0] = greeted[0] + both(cond, til != tile).astype(jnp.int32)
    for _, _, _, til, cond, _ in served_ends:
        greeted[0] = greeted[0] + both(cond, til != tile).astype(jnp.int32)
    for _, _, home, cond in end_homes:
        greeted[0] = greeted[0] + both(cond, home != tile).astype(jnp.int32)
    greeted[0] = greeted[0] + jnp.where(is_home, 3, 0)

    for copy in inputs:
        copy.wait()
    ext[8:136, 1] = res[...].astype(BF16)
    for b in range(3):
        ext[pl.ds(seam_rows, 8), b] = jnp.zeros((8, 8, 128), BF16)

    @pl.when(at_end)
    def _():
        for i in range(0, 144, 16):
            ext[i:i + 16, 2 * side] = jnp.zeros((16, 8, 128), BF16)
    xf[...] = res[pl.ds(120 * r, 8)].reshape(64, 128)
    for p in range(8):
        tr[p] = xf[pl.ds(p, 8, stride=8), :].astype(BF16)

    row_type = jnp.where(seam[0, panel, 1] >= 0, 1, 0)
    facts = []
    for slot in range(2):
        edge = 2 * slot + row_type
        facing_panel = jnp.maximum(seam[0, panel, edge], 0)
        facing = lax.rem(edge + 2 + seam[1, panel, edge], 4)
        rev = jnp.where(seam[2, panel, edge] > 0, 1, 0)
        flip = jnp.where((facing >= 2) == (slot == 1), 1, 0)
        pick = jnp.clip(lax.rem(facing_panel - panel + 3, 4), 0, 2)
        facts.append((pick, rev, flip))
    rowf = jnp.full((64, 128), row_type, jnp.int32) == 1
    to_second = [jnp.where(seam[0, panel, 2 + row_type] == lax.rem(panel + step, PANELS), 1, 0)
                 for step in range(1, PANELS)]

    pl.semaphore_wait(barrier, greeted[0])

    def remote(src, dst, slot, rslot, pan, til):
        return pltpu.make_async_remote_copy(
            src_ref=src, dst_ref=dst, send_sem=send_sem.at[slot], recv_sem=recv_sem.at[rslot],
            device_id=(pan, til), device_id_type=MESH)

    used = [0]
    stand_in = {64: corner_in.at[pl.ds(0, 64)], 16: corner_in.at[pl.ds(0, 16)], 112: corner_in.at[pl.ds(0, 112)], 4: tr.at[pl.ds(0, 4)], 8: tr, 128: corner_in, 2: cross_out.at[0]}

    def send(cond, src, dst, rslot, til, pan=None):
        pan = panel if pan is None else pan
        slot = used[0]
        used[0] += 1

        def now():
            remote(src, dst, slot, rslot, pan, til).start()
        if cond is None:
            now()
        else:
            pl.when(cond)(now)
        books[-1][1].append((cond, slot, src.shape[0]))

    def deliver(cond, src, dst, rslot, til):
        send(both(cond, til != tile), src, dst, rslot, til)

        @pl.when(both(cond, til == tile))
        def _():
            dst[...] = src[...]
        _, slot, size = books[-1][1].pop()
        books[-1][1].append(((cond, til), slot, size))

    books = [(None, [])]

    def block(cond, body):
        books.append((cond, []))
        pl.when(cond)(body)
        books.append((None, []))

    def sent():
        def settle(entries):
            for cond, slot, size in entries:
                if isinstance(cond, tuple):
                    cond = both(cond[0], cond[1] != tile)
                ref = stand_in[size]

                def done():
                    remote(ref, ref, slot, 0, panel, tile).wait_send()
                if cond is None:
                    done()
                else:
                    pl.when(cond)(done)
        for cond, entries in books:
            if cond is None:
                settle(entries)
            else:
                pl.when(cond)(lambda: settle(entries))
        books[:] = [(None, [])]

    def arrived(cond, dst, rslot):
        def now():
            remote(dst, dst, 0, rslot, panel, tile).wait_recv()
        if cond is None:
            now()
        else:
            pl.when(cond)(now)

    def ends_in():
        for jj, piece, home, cond in end_homes:
            if 1 <= jj <= 16:
                deliver(yes, ext.at[pl.ds(8 * jj + 4 * piece, 4), 1], in_home.at[0, side, r],
                        IN_HOME + 2 * side + r, home)
    block(at_end, ends_in)
    for b, piece, home, cond in tile_homes:
        if b == 1:
            deliver(cond, tr.at[pl.ds(4 * piece, 4)], in_home.at[1, r, half],
                    IN_HOME + 4 + 2 * r + half, home)
    edge_src = ext.at[pl.ds(128 - 120 * r, 8), 1]
    send(None, edge_src, ext.at[pl.ds(136 * r, 8), 1], HALO, tid(other, c))
    send(has_right, edge_src, ext.at[pl.ds(136 * r, 8), 0], HALO + 1, tid(other, c + 1))
    send(has_left, edge_src, ext.at[pl.ds(136 * r, 8), 2], HALO + 2, tid(other, c - 1))
    for piece, first in ((pl.ds(8, 64), HALO + 3), (pl.ds(72, 64), HALO_REST)):
        send(has_right, ext.at[piece, 1], ext.at[piece, 0], first, tid(r, c + 1))
        send(has_left, ext.at[piece, 1], ext.at[piece, 2], first + 1, tid(r, c - 1))

    def turned(landed, slot):
        pick, rev, flip = facts[slot]
        yf[...] = landed[pick].astype(F32).reshape(64, 128)
        turn = 1 - 2 * flip
        for high in range(2):
            for i in range(4):
                first = jnp.where(rev == 1, 32 * (1 - high) + 8 * (3 - i), 32 * high + 8 * i) + 7 * flip
                for d in range(8):
                    zf[pl.ds(32 * high + 8 * i + d, 1), :] = yf[pl.ds(first + turn * d, 1), :]
        return zf[0:64, :]

    def cross(landing, source, first_slot):
        def out_of_panel():
            for step in range(1, PANELS):
                send(None, source.at[step - 1], landing.at[3 - step], first_slot + 3 - step, tile,
                     lax.rem(panel + step, PANELS))
        block(is_home, out_of_panel)

    def hand_out(landing, first_slot):
        for i in range(3):
            remote(landing.at[i], landing.at[i], 0, first_slot + i, panel, tile).wait_recv()
        for slot in range(2):
            value = turned(landing, slot)
            blank = jnp.zeros_like(value)
            row_out[slot] = jnp.where(rowf, value, blank).astype(BF16).reshape(2, 4, 8, 128)
            col_out[slot] = jnp.where(rowf, blank, value).astype(BF16).reshape(2, 4, 8, 128)

    for k in range(0, CELLS, 64):
        some = jnp.broadcast_to(weight[pl.ds(k, 64)].reshape(1, 64), (128, 64))
        wrep[pl.ds(k, 64), :] = jnp.transpose(some, (1, 0))
    for n in range(NSUB):
        pltpu.make_async_copy(inv_hbm.at[n], inv.at[n], inv_sem.at[n]).wait()

    @pl.when(at_end)
    def _():
        place = lax.broadcasted_iota(jnp.int32, (CELLS, 192), 0)
        want = lax.broadcasted_iota(jnp.int32, (CELLS, 192), 1)
        want = 24 * lax.div(want, 8) + lax.rem(want, 8) + 16 * side
        choose = jnp.where(place == want, 1.0, 0.0).astype(BF16)

        by_block = wide.reshape(24, 3, 8, 192)

        def gather(n, carry):
            found = jnp.dot(inv[n], choose, preferred_element_type=F32)
            ends[n] = found.astype(BF16)
            wide[...] = found
            facing_ends[n] = by_block[:, 2 * side].reshape(192, 192).astype(BF16)
            return carry
        lax.fori_loop(0, NSUB, gather, 0)

    came_rows = []
    for slot in range(2):
        for high in range(2):
            k = (LAST - mu) if high else mu
            came_rows.append((1, slot, high, tid(slot, k)))
            came_rows.append((0, slot, high, tid(high, LAST * slot)))

    @pl.when(is_home)
    def _():
        for kind, slot, high, til in came_rows:
            arrived(til != tile, in_home.at[kind, slot, high], IN_HOME + 4 * kind + 2 * slot + high)
        for step in range(3):
            cross_out[step] = in_home[row_type, to_second[step]]
    cross(cross_in, cross_out, CROSS)

    spread[...] = jnp.zeros_like(spread)

    arrived(None, ext.at[pl.ds(inner_rows, 8), 1], HALO)
    arrived(has_left, ext.at[pl.ds(inner_rows, 8), 0], HALO + 1)
    arrived(has_right, ext.at[pl.ds(inner_rows, 8), 2], HALO + 2)
    arrived(has_left, ext.at[pl.ds(8, 64), 0], HALO + 3)
    arrived(has_right, ext.at[pl.ds(8, 64), 2], HALO + 4)
    flat = ext.reshape(144 * 24, 128)

    def solve(n, carry):
        rows = pl.ds(pl.multiple_of(n * 192, 64), CELLS)
        solved = jnp.dot(inv[n], flat[rows, :], preferred_element_type=F32)
        spread[rows, :] += solved * wrep[...]
        return carry

    lax.fori_loop(0, FIRST, solve, 0, unroll=True)

    @pl.when(is_home)
    def _():
        hand_out(cross_in, CROSS)

    def ghosts_out():
        for slot, high, row, til, cond, at in served_ends:
            deliver(cond, col_out.at[slot, high], colg.at[pl.ds(at, 4)], COL_GHOST + at // 4, til)
        for slot, high, b, til, cond in served_rows:
            piece = (1 - part) if high else part
            deliver(cond, row_out.at[slot, high], rowg.at[pl.ds(8 * b + 4 * piece, 4)], ROW_GHOST + 2 * b + piece, til)
    block(is_home, ghosts_out)

    arrived(has_left, ext.at[pl.ds(72, 64), 0], HALO_REST)
    arrived(has_right, ext.at[pl.ds(72, 64), 2], HALO_REST + 1)
    lax.fori_loop(FIRST, NSUB, solve, 0, unroll=3)

    cube = spread.reshape(144, 3, 8, 128)
    clear = pl.ds(16 * other, 112)
    not_end = jnp.logical_not(at_end)

    def clear_rows():
        for b in range(2):
            for i in range(0, 112, 16):
                sides[b, pl.ds(16 * other + i, 16)] = cube[pl.ds(8 + 16 * other + i, 16), 2 * b].astype(BF16)

    @pl.when(not_end)
    def _():
        clear_rows()
    send(not_end, sides.at[0, clear], from_right.at[clear], HALO_BACK, tid(r, c - 1))
    send(not_end, sides.at[1, clear], from_left.at[clear], HALO_BACK + 1, tid(r, c + 1))

    end_cells = colg.reshape(144 * 8, 128)

    @pl.when(at_end)
    def _():
        for jj, piece, home, cond in end_homes:
            arrived(both(cond, home != tile), colg.at[pl.ds(8 * jj + 4 * piece, 4)], COL_GHOST + 2 * jj + piece)


    for b, piece, home, cond in tile_homes:
        arrived(both(cond, home != tile), rowg.at[pl.ds(8 * b + 4 * piece, 4)], ROW_GHOST + 2 * b + piece)
    zf[...] = rowg[...].astype(F32).reshape(192, 128)
    for i in range(8):
        rg[24 * i:24 * i + 24, :] = zf[pl.ds(i, 24, stride=8), :]

    @pl.when(r == 0)
    def _():
        more = jnp.dot(inv[0][:, 0:192], rg[...].astype(BF16), preferred_element_type=F32)
        spread[0:CELLS, :] += more * wrep[...]

    @pl.when(r == 1)
    def _():
        more = jnp.dot(inv[NSUB - 1][:, 384:CELLS], rg[...].astype(BF16), preferred_element_type=F32)
        spread[192 * (NSUB - 1):, :] += more * wrep[...]

    @pl.when(at_end)
    def _():
        edge_weight = wrep.reshape(24, 3, 8, 128)[:, 2 * side].reshape(192, 128)
        for i in range(0, 144, 16):
            colsum[8 * i:8 * i + 128, :] = cube[i:i + 16, 2 * side].reshape(128, 128)

        def add_first(n, carry):
            rows = pl.ds(pl.multiple_of(n * 64, 64), 192)
            colsum[rows, :] += jnp.dot(facing_ends[n], end_cells[rows, :], preferred_element_type=F32) * edge_weight
            return carry
        lax.fori_loop(0, NSUB, add_first, 0)

    def ends_back():
        for i in range(0, 144, 16):
            colb[i:i + 16] = colsum[8 * i:8 * i + 128, :].reshape(16, 8, 128).astype(BF16)
        for jj, piece, home, cond in end_homes:
            high = jnp.where(16 * r + jj - 1 >= 16, 1, 0)
            deliver(cond, colb.at[pl.ds(8 * jj + 4 * piece, 4)], col_back.at[side, high, r],
                    COL_BACK + 4 * side + 2 * high + r, home)
    block(at_end, ends_back)

    for p in range(24):
        rowt[p] = spread[pl.ds(24 * seam_rows + p, 8, stride=24), :].astype(BF16)
    for b, piece, home, cond in tile_homes:
        high = jnp.where(c + b - 1 >= 16, 1, 0)
        deliver(cond, rowt.at[pl.ds(8 * b + 4 * piece, 4)], row_back.at[r, high, b],
                ROW_BACK + 6 * r + 3 * high + b, home)

    @pl.when(at_end)
    def _():
        def add(n, carry):
            rows = pl.ds(pl.multiple_of(n * 192, 64), CELLS)
            some = end_cells[pl.ds(pl.multiple_of(n * 64, 64), 192), :]
            spread[rows, :] += jnp.dot(ends[n], some, preferred_element_type=F32) * wrep[...]
            return carry
        lax.fori_loop(0, NSUB, add, 0)

    for b in range(3):
        inners[b] = cube[pl.ds(inner_rows, 8), b].astype(BF16)
    send(None, inners.at[1], from_vert, HALO_BACK + 2, tid(other, c))
    send(has_left, inners.at[0], from_dr, HALO_BACK + 3, tid(other, c - 1))
    send(has_right, inners.at[2], from_dl, HALO_BACK + 4, tid(other, c + 1))
    for b in range(2):
        sides[b, pl.ds(112 * r, 16)] = cube[pl.ds(8 + 112 * r, 16), 2 * b].astype(BF16)
    late = pl.ds(112 * r, 16)
    send(has_left, sides.at[0, late], from_right.at[late], LATE_ROWS, tid(r, c - 1))
    send(has_right, sides.at[1, late], from_left.at[late], LATE_ROWS + 1, tid(r, c + 1))

    @pl.when(at_end)
    def _():
        clear_rows()
    send(both(at_end, has_left), sides.at[0, clear], from_right.at[clear], HALO_BACK, tid(r, c - 1))
    send(both(at_end, has_right), sides.at[1, clear], from_left.at[clear], HALO_BACK + 1, tid(r, c + 1))

    @pl.when(is_home)
    def _():
        for slot, high, b, til, cond in served_rows:
            arrived(both(cond, til != tile), row_back.at[slot, high, b], ROW_BACK + 6 * slot + 3 * high + b)
        for slot, high, row, til, cond, _ in served_ends:
            arrived(both(cond, til != tile), col_back.at[slot, high, row], COL_BACK + 4 * slot + 2 * high + row)
        for slot in range(2):
            for high in range(2):
                by_row = row_back[slot, high, 0].astype(F32) + row_back[slot, high, 1].astype(F32)
                by_row = by_row + row_back[slot, high, 2].astype(F32)
                by_col = col_back[slot, high, 0].astype(F32) + col_back[slot, high, 1].astype(F32)
                mask = jnp.full((4, 8, 128), row_type, jnp.int32) == 1
                in_home[0, slot, high] = jnp.where(mask, by_row, by_col).astype(BF16)
        for step in range(3):
            back_out[step] = in_home[0, to_second[step]]
    cross(back_in, back_out, CROSS_BACK)

    sent()

    @pl.when(is_home)
    def _():
        hand_out(back_in, CROSS_BACK)

    def sums_out():
        for slot, high, row, til, cond, at in served_ends:
            if row == high:
                pos = highpos if high else lowpos
                deliver(yes, col_out.at[slot, high], corner_in.at[pl.ds(pos, 4)], COL_OWN + pos // 4, til)
        for slot, high, b, til, cond in served_rows:
            if b == 1:
                piece = (1 - part) if high else part
                deliver(yes, row_out.at[slot, high], own_back.at[pl.ds(4 * piece, 4)], ROW_OWN + piece, til)
    block(is_home, sums_out)
    arrived(has_right, from_right.at[clear], HALO_BACK)
    arrived(has_left, from_left.at[clear], HALO_BACK + 1)
    arrived(has_right, from_right.at[late], LATE_ROWS)
    arrived(has_left, from_left.at[late], LATE_ROWS + 1)
    arrived(None, from_vert, HALO_BACK + 2)
    arrived(has_left, from_dl, HALO_BACK + 4)
    arrived(has_right, from_dr, HALO_BACK + 3)
    out[...] = cube[pl.ds(8, 128), 1]

    @pl.when(has_right)
    def _():
        out[...] += from_right[...].astype(F32)
        out[pl.ds(120 * other, 8)] += from_dr[...].astype(F32)

    @pl.when(has_left)
    def _():
        out[...] += from_left[...].astype(F32)
        out[pl.ds(120 * other, 8)] += from_dl[...].astype(F32)

    out[pl.ds(120 * other, 8)] += from_vert[...].astype(F32)

    for b, piece, home, cond in tile_homes:
        if b == 1:
            arrived(both(cond, home != tile), own_back.at[pl.ds(4 * piece, 4)], ROW_OWN + piece)
    xf[...] = own_back[...].astype(F32).reshape(64, 128)
    for i in range(8):
        out[120 * r + i] += xf[pl.ds(i, 8, stride=8), :]

    @pl.when(at_end)
    def _():
        for jj, piece, home, cond in end_homes:
            if 1 <= jj <= 16:
                arrived(home != tile, corner_in.at[pl.ds(8 * (jj - 1) + 4 * piece, 4)],
                        COL_OWN + 2 * (jj - 1) + piece)
        out[...] += corner_in[...].astype(F32)
    sent()


def local(residual, inverse, blend_weight, seam_table):
    def vmem(*shape, dtype=BF16):
        return pltpu.VMEM(shape, dtype)
    unit = (4, 8, 128)
    scratch = [
        pltpu.SMEM((3, PANELS, 4), jnp.int32),
        vmem(H, 8, 128, dtype=F32),
        vmem(CELLS, dtype=F32),
        vmem(NSUB, CELLS, CELLS),
        vmem(NSUB, CELLS, 192),
        vmem(NSUB, 192, 192),
        vmem(CELLS, 192, dtype=F32),
        vmem(144 * 8, 128, dtype=F32),
        vmem(CELLS, 128, dtype=F32),
        vmem(144, 3, 8, 128),
        vmem(144 * 24, 128, dtype=F32),
        vmem(144, 8, 128), vmem(144, 8, 128),
        vmem(2, H, 8, 128), vmem(3, 8, 8, 128),
        vmem(8, 8, 128),
        vmem(24, 8, 128),
        vmem(24, 8, 128),
        vmem(8, 8, 128),
        vmem(H, 8, 128),
        vmem(2, 2, 2, *unit),
        vmem(3, 2, *unit), vmem(3, 2, *unit),
        vmem(2, 2, *unit), vmem(2, 2, *unit),
        vmem(2, 2, 3, *unit),
        vmem(2, 2, 2, *unit),
        vmem(3, 2, *unit), vmem(3, 2, *unit),
        vmem(64, 128, dtype=F32),
        vmem(64, 128, dtype=F32),
        vmem(192, 128, dtype=F32),
        vmem(192, 128, dtype=F32),
        vmem(H, 8, 128), vmem(H, 8, 128),
        vmem(8, 8, 128), vmem(8, 8, 128), vmem(8, 8, 128),
        pltpu.SemaphoreType.DMA((3,)),
        pltpu.SemaphoreType.DMA((NSUB,)),
        pltpu.SemaphoreType.DMA((SENDS,)),
        pltpu.SemaphoreType.DMA((RECVS,)),
    ]
    given = (jnp.transpose(seam_table, (2, 0, 1)), residual[0, 0], inverse[0, 0], blend_weight)
    out = pl.pallas_call(
        kernel,
        out_shape=jax.ShapeDtypeStruct((H, 8, 128), F32),
        in_specs=[pl.BlockSpec(memory_space=pltpu.HBM)] * 4,
        out_specs=pl.BlockSpec(memory_space=pltpu.VMEM),
        scratch_shapes=scratch,
        compiler_params=pltpu.CompilerParams(
            collective_id=0, has_side_effects=True, vmem_limit_bytes=46 * 1024 * 1024),
        name="schwarz",
    )(*[pltpu.with_memory_space_constraint(a, pltpu.HBM) for a in given])
    return out[None, None]


def solution(mesh):
    placed = (P("panel", "tile", None, None, None), P("panel", "tile", None, None, None), P(), P())
    return jax.shard_map(
        local,
        mesh=mesh,
        in_specs=placed,
        out_specs=P("panel", "tile", None, None, None),
        check_vma=False,
    )
```
